32 devices in a mesh: lat: 16 (over z, y, core), lon: 2 (over x).
Axes of the slice: x: 2, y: 2, z: 4, core: 2. Of those that a mesh axis runs over, the one named last changes fastest.
Arguments:
- eastward_speed_face: float32 [72, 512, 256], P(None, 'lat', 'lon'), may hold values from -6 to 6
- northward_speed_face: float32 [72, 512, 256], P(None, 'lat', 'lon'), may hold values from -6 to 6
- stratum_extent_east_face: float32 [72, 512, 256], P(None, 'lat', 'lon'), may hold values from 0.5 to 2
- stratum_extent_north_face: float32 [72, 512, 256], P(None, 'lat', 'lon'), may hold values from 0.5 to 2
- northward_span_east_face: float32 [512, 256], P('lat', 'lon'), may hold values from 0.5 to 2
- eastward_span_north_face: float32 [512, 256], P('lat', 'lon'), may hold values from 0.5 to 2
- ocean_flag_east_face: int32 [72, 512, 256], P(None, 'lat', 'lon'), may hold values 0 or 1
- ocean_flag_north_face: int32 [72, 512, 256], P(None, 'lat', 'lon'), may hold values 0 or 1
- counterpart_across_seam: int32 [256], replicated, may hold values from 0 to 255, as said below
Outputs:
- eastward_speed_next: float32 [72, 512, 256], P(None, 'lat', 'lon')
- northward_speed_next: float32 [72, 512, 256], P(None, 'lat', 'lon')
The draws below stay inside these ranges and needn't reach their ends.
Inputs may be any that keep to these rules, and one draw needn't show every extreme that they name: counterpart_across_seam[i] = (p - 1 - i) mod 256 for one pivot p drawn anew in each draw; it is its own inverse.
All inputs are finite; a program needn't handle non-finite values. No bound on the sum of `ocean_flag_east_face` or of `ocean_flag_north_face` on one device may be relied on, other than what follows from the above.
Results may differ from the reference program's by a relative error of at most 0.00002.
Values sent between devices are 32-bit elements; how exact they have to be, the bound alone decides.
A program may use at most 128 MiB of HBM per device.

```python
import math
import jax
import jax.numpy as jnp
from jax import lax

STRATA_COUNT = 72
NORTHWARD_CELLS = 512
EASTWARD_CELLS = 256


def draw_counterpart_across_seam(key, part):
    pivot = jax.random.randint(jax.random.fold_in(key, 17), (), 0, EASTWARD_CELLS)
    columns = jnp.arange(EASTWARD_CELLS, dtype=jnp.int32)
    return ((pivot - 1 - columns) % EASTWARD_CELLS).astype(jnp.int32)


def touch_ends(values, rng, low, high):
    longest = values.shape.index(max(values.shape))
    spots = []
    for shift in (0, 1):
        where = [jax.random.randint(jax.random.fold_in(rng, axis), (), 0, length) for axis, length in enumerate(values.shape)]
        where[longest] = (where[longest] + shift) % values.shape[longest]
        spots.append(tuple(where))
    return values.at[spots[0]].set(low).at[spots[1]].set(high)


def shard_levels(rng, shape, pieces, least, top_value):
    def one(dim, parts):
        draws = jax.random.uniform(jax.random.fold_in(jax.random.fold_in(rng, 6), dim), (parts,), jnp.float32, least / len(pieces), top_value / len(pieces))
        return jnp.repeat(jnp.exp(draws), shape[dim] // parts).reshape((-1,) + (1,) * (len(shape) - dim - 1))

    loudness = one(*pieces[0])
    for cut in pieces[1:]:
        loudness = loudness * one(*cut)
    return loudness


def centred(key, shape, scale, most, pieces=(), kind=jnp.bfloat16):
    loudness = shard_levels(key, shape, pieces, -0.22, 0.18) if pieces else 1.0
    values = jax.random.normal(key, shape, jnp.float32) * scale * loudness
    return jnp.minimum(jnp.maximum(values, -most), most).astype(kind)


def setup_inputs(seed: int = 0) -> dict:
    key_of = jax.random.split(jax.random.key(seed), 10)
    return {
        "eastward_speed_face": centred(key_of[0], (STRATA_COUNT, NORTHWARD_CELLS, EASTWARD_CELLS), 1.0, 6.0, ((1, 16), (2, 2)), jnp.float32),
        "northward_speed_face": centred(key_of[1], (STRATA_COUNT, NORTHWARD_CELLS, EASTWARD_CELLS), 1.0, 6.0, ((1, 16), (2, 2)), jnp.float32),
        "stratum_extent_east_face": jnp.clip(jnp.exp(math.log(2.0) - 1.3862944 * jax.random.uniform(key_of[2], (STRATA_COUNT, NORTHWARD_CELLS, EASTWARD_CELLS), jnp.float32) ** shard_levels(key_of[2], (STRATA_COUNT, NORTHWARD_CELLS, EASTWARD_CELLS), ((1, 16), (2, 2)), -0.2, 0.2)), 0.5, 2.0),
        "stratum_extent_north_face": jnp.clip(jnp.exp(math.log(2.0) - 1.3862944 * jax.random.uniform(key_of[3], (STRATA_COUNT, NORTHWARD_CELLS, EASTWARD_CELLS), jnp.float32) ** shard_levels(key_of[3], (STRATA_COUNT, NORTHWARD_CELLS, EASTWARD_CELLS), ((1, 16), (2, 2)), -0.2, 0.2)), 0.5, 2.0),
        "northward_span_east_face": jnp.clip(jnp.exp(math.log(2.0) - 1.3862944 * jax.random.uniform(key_of[4], (NORTHWARD_CELLS, EASTWARD_CELLS), jnp.float32) ** shard_levels(key_of[4], (NORTHWARD_CELLS, EASTWARD_CELLS), ((0, 16), (1, 2)), -0.2, 0.2)), 0.5, 2.0),
        "eastward_span_north_face": jnp.clip(jnp.exp(math.log(2.0) - 1.3862944 * jax.random.uniform(key_of[5], (NORTHWARD_CELLS, EASTWARD_CELLS), jnp.float32) ** shard_levels(key_of[5], (NORTHWARD_CELLS, EASTWARD_CELLS), ((0, 16), (1, 2)), -0.2, 0.2)), 0.5, 2.0),
        "ocean_flag_east_face": touch_ends((jax.random.randint(key_of[6], (STRATA_COUNT, NORTHWARD_CELLS, EASTWARD_CELLS), 0, 4) < 3).astype(jnp.int32), jax.random.fold_in(key_of[6], 1), 0, 1),
        "ocean_flag_north_face": touch_ends((jax.random.randint(key_of[7], (STRATA_COUNT, NORTHWARD_CELLS, EASTWARD_CELLS), 0, 4) < 3).astype(jnp.int32), jax.random.fold_in(key_of[7], 1), 0, 1),
        "counterpart_across_seam": draw_counterpart_across_seam(jax.random.fold_in(key_of[9], 71), 0),
    }


time_step = 0.2


def interp(a, b, c, d):
    return (7.0 * (b + c) - (a + d)) / 12.0


def advect(umv, vmv, tuv, tvv, rows, cols):
    def cx(field, ro, co):
        return field[..., ro:ro + rows, co:co + cols + 1]

    def ry(field, ro, co):
        return field[..., ro:ro + rows + 1, co:co + cols]

    fut = 0.5 * (cx(tuv, 2, 1) + cx(tuv, 2, 2)) * interp(cx(umv, 2, 0), cx(umv, 2, 1), cx(umv, 2, 2), cx(umv, 2, 3))
    vface = ry(tvv, 1, 2)
    fvf = 0.5 * (vface + ry(tvv, 1, 3)) * interp(ry(umv, 0, 2), ry(umv, 1, 2), ry(umv, 2, 2), ry(umv, 3, 2))
    fuf = 0.5 * (cx(tuv, 2, 1) + cx(tuv, 3, 1)) * interp(cx(vmv, 2, 0), cx(vmv, 2, 1), cx(vmv, 2, 2), cx(vmv, 2, 3))
    fvt = 0.5 * (vface + ry(tvv, 2, 2)) * interp(ry(vmv, 0, 2), ry(vmv, 1, 2), ry(vmv, 2, 2), ry(vmv, 3, 2))
    trend_u = -((fut[..., 1:] - fut[..., :-1]) + (fvf[..., 1:, :] - fvf[..., :-1, :]))
    trend_v = -((fuf[..., 1:] - fuf[..., :-1]) + (fvt[..., 1:, :] - fvt[..., :-1, :]))
    return trend_u, trend_v


def extend(field, counterpart_across_seam):
    north = -field[-2:, :][::-1, :][:, counterpart_across_seam]
    south = jnp.zeros((2, field.shape[1]), jnp.float32)
    padded = jnp.concatenate([south, field, north], axis=0)
    return jnp.concatenate([padded[:, -2:], padded, padded[:, :2]], axis=1)


def reference(eastward_speed_face, northward_speed_face, stratum_extent_east_face, stratum_extent_north_face, northward_span_east_face, eastward_span_north_face, ocean_flag_east_face, ocean_flag_north_face, counterpart_across_seam):
    def stratum_index(items):
        uk, vk, e3uk, e3vk, umk, vmk = items
        um = umk.astype(jnp.float32) * uk
        vm = vmk.astype(jnp.float32) * vk
        volu = northward_span_east_face * e3uk
        volv = eastward_span_north_face * e3vk
        tu = volu * um
        tv = volv * vm
        ext = [extend(f, counterpart_across_seam) for f in (um, vm, tu, tv)]
        trend_u, trend_v = advect(ext[0], ext[1], ext[2], ext[3], um.shape[0], um.shape[1])
        u_new = umk.astype(jnp.float32) * (um + time_step * trend_u / volu)
        v_new = vmk.astype(jnp.float32) * (vm + time_step * trend_v / volv)
        return u_new, v_new

    eastward_speed_next, northward_speed_next = lax.map(stratum_index, (eastward_speed_face, northward_speed_face, stratum_extent_east_face, stratum_extent_north_face, ocean_flag_east_face, ocean_flag_north_face))
    return eastward_speed_next, northward_speed_next
```

```python
import functools

import jax
import jax.numpy as jnp
from jax import lax
from jax.experimental import pallas as pl
from jax.experimental.pallas import tpu as pltpu
from jax.sharding import PartitionSpec as P

time_step = 0.2
scale = -time_step / 24.0
lanes = 128
group = 8
pad = 8
MESH = pl.DeviceIdType.MESH
f32 = jnp.float32


def chunk_count(levels, per):
    count = levels // per
    return next(c for c in (3, 2, 1) if count % c == 0)


def roll(x, shift):
    return pltpu.roll(x, shift % lanes, 1)


def vroll(x, shift):
    return pltpu.roll(x, shift % group, 0)


def q(a, b, c, d):
    return 7.0 * (b + c) - (a + d)


def exchange_kernel(
    nlat, nlon, levels, rows,
    u_hbm, v_hbm, eu_hbm, ev_hbm, su_hbm, sv_hbm, mu_hbm, mv_hbm,
    u_part, v_part, low_own, high_own, keep, side, up_in, down_in, corner_u, corner_v, band,
    u_in, v_in, eu_in, ev_in, su_in, sv_in, mu_in, mv_in,
    edge_f, edge_m, um_n, vm_n, tv_n, cu_n, cv_n, um_t, vm_t, tu_t, ts_t,
    pack_own, pack_in, edge_own, edge_in, corner_u_own, corner_v_own, fix,
    edge_sem, load_sem, span_sem, up_send, up_recv, down_send, down_recv,
    lon_send, lon_recv, side_send, side_recv, diag_send, diag_recv, band_send, band_recv,
):
    per = lanes // rows
    tall = rows // group
    blocks = levels // per
    chunks = chunk_count(levels, per)
    depth = levels // chunks
    blocks_in = blocks // chunks
    groups = levels // group
    pitch = rows + pad
    lat = lax.axis_index("lat")
    lon = lax.axis_index("lon")
    right = lax.rem(lon + 1, nlon)
    left = lax.rem(lon + nlon - 1, nlon)
    has_up = lat < nlat - 1
    has_down = lat > 0
    sides = 1 if nlon == 2 else 2
    picked = (0, 1, rows - 2, rows - 1)

    edges = [
        pltpu.make_async_copy(a.at[:, r, :], b.at[k, e], edge_sem.at[4 * s + e])
        for s, (a, b, k) in enumerate((
            (u_hbm, edge_f, 0), (mu_hbm, edge_m, 0), (v_hbm, edge_f, 1),
            (mv_hbm, edge_m, 1), (eu_hbm, edge_f, 2), (ev_hbm, edge_f, 3),
        ))
        for e, r in enumerate(picked)
    ]
    spans = [
        pltpu.make_async_copy(su_hbm, su_in, span_sem.at[0]),
        pltpu.make_async_copy(sv_hbm, sv_in, span_sem.at[1]),
    ]
    pairs = (
        (u_hbm, u_in), (mu_hbm, mu_in), (eu_hbm, eu_in),
        (v_hbm, v_in), (mv_hbm, mv_in), (ev_hbm, ev_in),
    )
    loads = [
        [
            pltpu.make_async_copy(
                a.at[pl.ds(c * depth, depth)], b.at[pl.ds(c * depth, depth)], load_sem.at[c, k]
            )
            for k, (a, b) in enumerate(pairs)
        ]
        for c in range(chunks)
    ]
    for copy in spans + edges:
        copy.start()
    for per_chunk in loads:
        for copy in per_chunk:
            copy.start()

    barrier = pltpu.get_barrier_semaphore()

    def greet(where):
        pl.semaphore_signal(barrier, inc=1, device_id=where, device_id_type=MESH)

    greet((lat, right))
    if nlon > 2:
        greet((lat, left))

    @pl.when(has_up)
    def _():
        greet((lat + 1, lon))
        greet((lat + 1, left))

    @pl.when(has_down)
    def _():
        greet((lat - 1, lon))
        greet((lat - 1, right))

    if nlon > 3:
        @pl.when(lat == nlat - 1)
        def _():
            for d in range(2, nlon - 1):
                greet((lat, lax.rem(lon + d, nlon)))

    def arrive():
        @pl.when(lat == 0)
        def _():
            pl.semaphore_wait(barrier, sides + 2)

        @pl.when(has_up & has_down)
        def _():
            pl.semaphore_wait(barrier, sides + 4)

        @pl.when(lat == nlat - 1)
        def _():
            pl.semaphore_wait(barrier, sides + 2 + max(nlon - 3, 0))

    def remote(src, dst, send, recv, where):
        return pltpu.make_async_remote_copy(
            src_ref=src, dst_ref=dst, send_sem=send, recv_sem=recv,
            device_id=where, device_id_type=MESH,
        )

    def up_copy():
        return remote(high_own.at[pl.ds(0, 5)], up_in, up_send, up_recv, (lat + 1, lon))

    def down_copy():
        return remote(low_own, down_in, down_send, down_recv, (lat - 1, lon))

    def lon_copies(c):
        return [
            remote(
                pack_own.at[k, c], pack_in.at[k, c],
                lon_send.at[c, k], lon_recv.at[c, k], (lat, target),
            )
            for k, target in enumerate((right, left))
        ]

    def side_copies():
        return [
            remote(edge_own, edge_in.at[k], side_send.at[k], side_recv.at[k], (lat, target))
            for k, target in enumerate((right, left))
        ]

    def corner_down():
        return remote(
            corner_u_own, corner_u, diag_send.at[0], diag_recv.at[0], (lat - 1, right)
        )

    def corner_up():
        return remote(
            corner_v_own, corner_v, diag_send.at[1], diag_recv.at[1], (lat + 1, left)
        )

    def band_copy(d):
        return remote(
            high_own, band.at[lon], band_send.at[d], band_recv.at[d],
            (lat, lax.rem(lon + d, nlon)),
        )

    def band_arrival(d):
        origin = lax.rem(lon + nlon - d, nlon)
        return remote(
            high_own, band.at[origin], band_send.at[d], band_recv.at[d],
            (lat, lax.rem(lon + d, nlon)),
        )

    lane = lax.broadcasted_iota(jnp.int32, (group, lanes), 1)
    sub = lax.broadcasted_iota(jnp.int32, (group, lanes), 0)
    zero = jnp.zeros((group, lanes), f32)

    def clear(l, carry):
        for ref in (um_n, vm_n):
            ref[pl.ds(pl.multiple_of(l * pitch, group), group), :] = zero
        return carry

    lax.fori_loop(0, levels + 1, clear, 0)

    @pl.when(lat == 0)
    def _():
        up_in[...] = jnp.zeros((5, levels, lanes), f32)
        corner_v[...] = zero

    for copy in spans + edges:
        copy.wait()

    def edge_step(g, carry):
        part = pl.ds(pl.multiple_of(g * group, group), group)
        um, vm, tu, tv = [], [], [], []
        for e, r in enumerate(picked):
            mu = edge_m[0, e, part, :].astype(f32)
            mv = edge_m[1, e, part, :].astype(f32)
            um.append(mu * edge_f[0, e, part, :])
            vm.append(mv * edge_f[1, e, part, :])
            vol_u = su_in[pl.ds(r, 1), :] * edge_f[2, e, part, :]
            vol_v = sv_in[pl.ds(r, 1), :] * edge_f[3, e, part, :]
            tu.append(vol_u * um[e])
            tv.append(vol_v * vm[e])
            keep[e, part, :] = mu * scale / vol_u
            keep[4 + e, part, :] = mv * scale / vol_v
        for k, x in enumerate((um[0], um[1], vm[0], vm[1], tu[0], tv[0])):
            low_own[k, part, :] = x
        for k, x in enumerate((um[2], um[3], vm[2], vm[3], tv[3], tu[3])):
            high_own[k, part, :] = x
            band[lon, k, part, :] = x
        keep[8, part, :] = tv[1]
        keep[9, part, :] = tv[2]
        return carry

    lax.fori_loop(0, groups, edge_step, 0)
    arrive()

    @pl.when(has_down)
    def _():
        down_copy().start()

    @pl.when(has_up)
    def _():
        up_copy().start()

    @pl.when(lat == nlat - 1)
    def _():
        for d in range(1, nlon):
            band_copy(d).start()

    first, second, ring = zero, zero, zero
    for g in range(groups):
        part = pl.ds(g * group, group)
        first = jnp.where(lane == g, roll(low_own[4, part, :], g + 1), first)
        tv_top = high_own[4, part, :]
        second = jnp.where(lane == g, roll(tv_top, g), second)
        ring = jnp.where(lane // 4 == g, roll(high_own[3, part, :], 4 * g + 2), ring)
        for k, x in enumerate((low_own[5, part, :], keep[9, part, :], tv_top)):
            ring = jnp.where(lane == 64 + 4 * g + k, roll(x, 64 + 4 * g + k), ring)
    corner_u_own[...] = first
    corner_v_own[...] = second
    edge_own[...] = ring
    for copy in side_copies():
        copy.start()

    @pl.when(has_down)
    def _():
        corner_down().start()

    @pl.when(has_up)
    def _():
        corner_up().start()

    def prepare(block, c):
        um_b, vm_b, tu_b, ts_b, tv_b = [], [], [], [], []
        for s in range(per):
            l = block * per + s
            base = pl.multiple_of(l * pitch + pad, group)
            tus = []
            for b in range(tall):
                at = pl.ds(b * group, group)
                mu = mu_in[l, at, :].astype(f32)
                mv = mv_in[l, at, :].astype(f32)
                um = mu * u_in[l, at, :]
                vm = mv * v_in[l, at, :]
                vol_u = su_in[at, :] * eu_in[l, at, :]
                vol_v = sv_in[at, :] * ev_in[l, at, :]
                tv = vol_v * vm
                tus.append(vol_u * um)
                um_n[pl.ds(base + b * group, group), :] = um
                vm_n[pl.ds(base + b * group, group), :] = vm
                tv_n[l, at, :] = tv
                cu_n[l, at, :] = mu * scale / vol_u
                cv_n[l, at, :] = mv * scale / vol_v
                um_b.append(um)
                vm_b.append(vm)
                tv_b.append(tv)
            turned = [vroll(x, -1) for x in tus] + [zero]
            for b in range(tall):
                ts_b.append(tus[b] + jnp.where(sub == group - 1, turned[b + 1], turned[b]))
            tu_b += tus
        here = block - c * blocks_in
        own = pl.ds(here, 1)

        def flip(tiles):
            return jnp.concatenate(tiles, axis=0).T

        for x, ref, west, east in (
            (flip(um_b), um_t, 0, 0), (flip(vm_b), vm_t, 2, 2),
        ):
            ref[block, pl.ds(pad, lanes), :] = x
            for k in range(2):
                pack_own[0, c, west + k, own, :] = x[lanes - 2 + k:lanes - 1 + k]
                pack_own[1, c, east + k, own, :] = x[k:k + 1]
        x = flip(tu_b)
        tu_t[block, pl.ds(pad, lanes), :] = x
        pack_own[0, c, 4, own, :] = x[lanes - 1:]
        pack_own[1, c, 4, own, :] = x[:1]
        x = flip(ts_b)
        ts_t[block, pl.ds(pad, lanes), :] = x
        pack_own[0, c, 5, own, :] = x[lanes - 1:]
        pack_own[1, c, 5, own, :] = flip(tv_b)[:1]

    def inside(block):
        for s in range(per):
            l = block * per + s
            base = l * pitch + pad

            def um(b, shift):
                return um_n[pl.ds(base + b * group + shift, group), :]

            def vm(b, shift):
                return vm_n[pl.ds(base + b * group + shift, group), :]

            f, w, tv_turned = [], [], []
            for b in range(tall):
                at = pl.ds(b * group, group)
                tv = tv_n[l, at, :]
                tv_turned.append(vroll(tv, 1))
                below = jnp.where(sub == 0, tv_turned[b - 1] if b else zero, tv_turned[b])
                f.append((tv + roll(tv, -1)) * q(um(b, -1), um(b, 0), um(b, 1), um(b, 2)))
                cross = (below + tv) * q(vm(b, -2), vm(b, -1), vm(b, 0), vm(b, 1))
                w.append(jnp.where(sub == 0, 0.0, cross) if b == 0 else cross)
            f_turned = [vroll(x, 1) for x in f]
            w_turned = [vroll(x, -1) for x in w] + [zero]
            for b in range(tall):
                at = pl.ds(b * group, group)
                below = jnp.where(sub == 0, f_turned[b - 1] if b else zero, f_turned[b])
                above = jnp.where(sub == group - 1, w_turned[b + 1], w_turned[b])
                u_part[l, at, :] = um(b, 0) + cu_n[l, at, :] * (f[b] - below)
                v_part[l, at, :] = vm(b, 0) + cv_n[l, at, :] * (above - w[b])

    slot = lax.broadcasted_iota(jnp.int32, (blocks_in, lanes), 1) % rows

    def lane_fix(c):
        own = pack_own[0, c, 1]

        def shifted(x, by):
            keep_it = (slot + by >= 0) & (slot + by < rows)
            return jnp.where(keep_it, pltpu.roll(x, (-by) % lanes, 1), 0.0)

        flux = (pack_in[1, c, 5] - pack_own[1, c, 5]) * q(
            shifted(own, -1), own, shifted(own, 1), shifted(own, 2)
        )
        fix[c] = flux - shifted(flux, -1)

    def across(block, c):
        here = pl.ds(block - c * blocks_in, 1)
        for ref, at in ((um_t, 0), (vm_t, 2)):
            for k in range(2):
                ref[block, pl.ds(pad - 2 + k, 1), :] = pack_in[0, c, at + k, here, :]
                ref[block, pl.ds(pad + lanes + k, 1), :] = pack_in[1, c, at + k, here, :]
        tu_t[block, pl.ds(pad - 1, 1), :] = pack_in[0, c, 4, here, :]
        tu_t[block, pl.ds(pad + lanes, 1), :] = pack_in[1, c, 4, here, :]
        ts_t[block, pl.ds(pad - 1, 1), :] = pack_in[0, c, 5, here, :]

        def read(ref, i):
            return ref[block, pl.ds(pad + i, group), :]

        def west(i):
            return (read(tu_t, i - 1) + read(tu_t, i)) * q(*[read(um_t, i + k) for k in (-2, -1, 0, 1)])

        def east(i):
            return read(ts_t, i) * q(*[read(vm_t, i + k) for k in (-1, 0, 1, 2)])

        count = lanes // group
        fs = [west(i * group) for i in range(count)]
        gs = [east(i * group) for i in range(count)]
        f_turned = [vroll(x, -1) for x in fs] + [west(lanes - group + 1)]
        g_turned = [east(-1)] + [vroll(x, 1) for x in gs]
        du = [
            jnp.where(sub == group - 1, f_turned[i + 1], f_turned[i]) - fs[i] for i in range(count)
        ]
        dv = [gs[i] - jnp.where(sub == 0, g_turned[i], g_turned[i + 1]) for i in range(count)]
        du[-1] = du[-1] + jnp.where(sub == group - 1, fix[c, here, :], 0.0)
        du = jnp.concatenate(du, axis=0).T
        dv = jnp.concatenate(dv, axis=0).T
        for s in range(per):
            l = block * per + s
            for b in range(tall):
                at = pl.ds(b * group, group)
                k = (s * tall + b) * group
                u_part[l, at, :] = u_part[l, at, :] + cu_n[l, at, :] * du[k:k + group]
                v_part[l, at, :] = v_part[l, at, :] + cv_n[l, at, :] * dv[k:k + group]

    def every(body, c):
        def run(i, carry):
            body(i)
            return carry

        lax.fori_loop(c * blocks_in, (c + 1) * blocks_in, run, 0)

    for c in range(chunks):
        for copy in loads[c]:
            copy.wait()
        every(lambda i: prepare(i, c), c)
        for copy in lon_copies(c):
            copy.start()
    for c in range(chunks):
        every(inside, c)

    for copy in side_copies():
        copy.wait()
    for g in range(groups):
        part = pl.ds(g * group, group)
        from_left, from_right = edge_in[0], edge_in[1]
        for k, x in enumerate((low_own[5, part, :], keep[9, part, :], high_own[4, part, :])):
            halo = roll(from_right, -(64 + 4 * g + k))
            side[k, part, :] = x + roll(jnp.where(lane == 0, halo, x), -1)
        vm = high_own[3, part, :]
        halo = roll(jnp.where(lane % 4 < 2, from_left, from_right), -(4 * g + 2))
        w2 = roll(jnp.where(lane >= lanes - 2, halo, vm), 2)
        w1 = roll(jnp.where(lane == lanes - 1, halo, vm), 1)
        e1 = roll(jnp.where(lane == 0, halo, vm), -1)
        e2 = roll(jnp.where(lane < 2, halo, vm), -2)
        side[3, part, :] = q(w2, w1, vm, e1)
        side[4, part, :] = q(w1, vm, e1, e2)

    for c in range(chunks):
        for copy in lon_copies(c):
            copy.wait()
        lane_fix(c)
        every(lambda i: across(i, c), c)

    @pl.when(has_down)
    def _():
        down_copy().wait_send()
        corner_down().wait_send()
        up_copy().wait_recv()
        corner_up().wait_recv()

    @pl.when(has_up)
    def _():
        up_copy().wait_send()
        corner_up().wait_send()
        down_copy().wait_recv()
        corner_down().wait_recv()

    @pl.when(lat == nlat - 1)
    def _():
        for d in range(1, nlon):
            band_copy(d).wait_send()
            band_arrival(d).wait_recv()


def finish_kernel(
    nlat, nlon, levels, rows,
    fold_ref, u_part, v_part, low_own, high_own, keep, side, up_in, down_in, corner_u, corner_v, band,
    u_out, v_out,
    high, high_left, u_low, u_high, v_low, v_high, sem,
):
    lat = lax.axis_index("lat")
    lon = lax.axis_index("lon")
    groups = levels // group
    width = nlon * lanes
    lane = lax.broadcasted_iota(jnp.int32, (group, lanes), 1)
    middle = pl.ds(group, rows - 2 * group)
    low = pl.ds(0, group)
    top = pl.ds(rows - group, group)
    first = [
        pltpu.make_async_copy(a.at[:, middle], b.at[:, middle], sem.at[k])
        for k, (a, b) in enumerate(((u_part, u_out), (v_part, v_out)))
    ]
    for copy in first:
        copy.start()

    @pl.when(lat == nlat - 1)
    def _():
        start = fold_ref[0]
        own = lax.rem(start - lon * lanes - lane + 2 * width, width)
        before = jnp.zeros_like(lane) + lax.rem(start - lon * lanes + 1 + 2 * width, width)

        def pick(k, part, index):
            block = index // lanes
            spot = index % lanes
            got = jnp.zeros((group, lanes), f32)
            for b in range(nlon):
                taken = jnp.take_along_axis(
                    band[b, k, part, :], spot, axis=1, mode="promise_in_bounds"
                )
                got = jnp.where(block == b, taken, got)
            return -got

        for g in range(groups):
            part = pl.ds(g * group, group)
            for k, source in enumerate((1, 0, 3, 2, 5, 4)):
                high[k, part, :] = pick(source, part, own)
            high_left[part, :] = pick(5, part, before)

    @pl.when(lat < nlat - 1)
    def _():
        for g in range(groups):
            part = pl.ds(g * group, group)
            for k in range(6):
                high[k, part, :] = down_in[k, part, :]
            high_left[part, :] = roll(corner_u[...], lanes - 1 - g)

    def copy_tiles(l, carry):
        for source, a, b in ((u_part, u_low, u_high), (v_part, v_low, v_high)):
            a[l] = source[l, low, :]
            b[l] = source[l, top, :]
        return carry

    lax.fori_loop(0, levels, copy_tiles, 0, unroll=8)

    views = [ref.reshape(levels * group, lanes) for ref in (u_low, u_high, v_low, v_high)]

    def add(view, g, row, value):
        at = pl.ds(g * group * group + row, group, stride=group)
        view[at, :] = view[at, :] + value

    for g in range(groups):
        part = pl.ds(g * group, group)
        um0, um1, vm0, vm1, _, tv0 = [low_own[k, part, :] for k in range(6)]
        vm30, vm31, tv31 = [high_own[k, part, :] for k in (2, 3, 4)]
        um_2, um_1, vm_2, vm_1, tv_1 = [up_in[k, part, :] for k in range(5)]
        um32, um33, vm32, vm33, tu32, tv32 = [high[k, part, :] for k in range(6)]
        cu0, cu1, cu30, cu31, cv0, cv1, cv30, cv31, tv1, tv30 = [keep[k, part, :] for k in range(10)]
        v0, v30, v31, q_west, q_east = [side[k, part, :] for k in range(5)]

        face = tv_1 + roll(jnp.where(lane == 0, roll(corner_v[...], -g), tv_1), -1)
        f_low = face * q(um_2, um_1, um0, um1)
        d0 = v0 * um_1
        add(views[0], g, 0, -cu0 * (d0 + f_low))
        add(views[0], g, 1, cu1 * d0)
        w_low = (tv_1 + tv0) * q(vm_2, vm_1, vm0, vm1)
        d0 = (tv0 + tv1) * vm_1
        add(views[2], g, 0, -cv0 * (d0 + w_low))
        add(views[2], g, 1, cv1 * d0)
        d30 = v30 * um32
        add(views[1], g, group - 2, -cu30 * d30)
        add(views[1], g, group - 1, cu31 * (v31 * (7.0 * um32 - um33) + d30))
        d30 = (tv30 + tv31) * vm32
        w_high = (tv31 + tv32) * q(vm30, vm31, vm32, vm33)
        tu_west = roll(jnp.where(lane == lanes - 1, high_left[part, :], tu32), 1)
        add(views[3], g, group - 2, -cv30 * d30)
        add(views[3], g, group - 1, cv31 * (w_high + d30 + (tu32 * q_east - tu_west * q_west)))

    last = [
        pltpu.make_async_copy(a, b.at[:, at], sem.at[2 + k])
        for k, (a, b, at) in enumerate((
            (u_low, u_out, low), (u_high, u_out, top), (v_low, v_out, low), (v_high, v_out, top),
        ))
    ]
    for copy in last:
        copy.start()
    for copy in first + last:
        copy.wait()


def local(nlat, nlon, u, v, eu, ev, su, sv, mu, mv, fold):
    u, v, eu, ev, su, sv, mu, mv = [
        pltpu.with_memory_space_constraint(x, pltpu.HBM) for x in (u, v, eu, ev, su, sv, mu, mv)
    ]
    levels, rows, _ = u.shape
    per = lanes // rows
    blocks = levels // per
    chunks = chunk_count(levels, per)
    blocks_in = blocks // chunks
    pitch = rows + pad
    vmem = pl.BlockSpec(memory_space=pltpu.VMEM)
    hbm = pl.BlockSpec(memory_space=pltpu.HBM)
    block = (levels, rows, lanes)
    line = (levels, lanes)
    shapes = [
        block, block,
        (6,) + line, (6,) + line, (10,) + line, (5,) + line, (5,) + line, (6,) + line,
        (group, lanes), (group, lanes), (nlon, 6) + line,
    ]
    tall = (levels * pitch + pad, lanes)
    turned = (blocks, lanes + 2 * pad, lanes)
    packs = (2, chunks, 6, blocks_in, lanes)
    dma = pltpu.SemaphoreType.DMA
    V = pltpu.VMEM
    fields = pl.pallas_call(
        functools.partial(exchange_kernel, nlat, nlon, levels, rows),
        out_shape=[V(s, f32) for s in shapes],
        in_specs=[hbm] * 8,
        out_specs=[vmem] * len(shapes),
        scratch_shapes=[
            V(block, f32), V(block, f32), V(block, f32), V(block, f32),
            V((rows, lanes), f32), V((rows, lanes), f32),
            V(block, jnp.int32), V(block, jnp.int32),
            V((4, 4) + line, f32), V((2, 4) + line, jnp.int32),
            V(tall, f32), V(tall, f32), V(block, f32), V(block, f32), V(block, f32),
            V(turned, f32), V(turned, f32), V(turned, f32), V(turned, f32),
            V(packs, f32), V(packs, f32),
            V((group, lanes), f32), V((2, group, lanes), f32),
            V((group, lanes), f32), V((group, lanes), f32),
            V((chunks, blocks_in, lanes), f32),
            dma((24,)), dma((chunks, 6)), dma((2,)),
            dma, dma, dma, dma,
            dma((chunks, 2)), dma((chunks, 2)), dma((2,)), dma((2,)), dma((2,)), dma((2,)),
            dma((nlon,)), dma((nlon,)),
        ],
        compiler_params=pltpu.CompilerParams(
            collective_id=0, has_side_effects=True, vmem_limit_bytes=36 * 1024 * 1024
        ),
        name="exchange",
    )(u, v, eu, ev, su, sv, mu, mv)
    strip = (levels, group, lanes)
    result = pl.pallas_call(
        functools.partial(finish_kernel, nlat, nlon, levels, rows),
        out_shape=[jax.ShapeDtypeStruct(block, f32)] * 2,
        in_specs=[pl.BlockSpec(memory_space=pltpu.SMEM)] + [vmem] * len(shapes),
        out_specs=[hbm] * 2,
        scratch_shapes=[
            V((6,) + line, f32), V(line, f32),
            V(strip, f32), V(strip, f32), V(strip, f32), V(strip, f32),
            dma((6,)),
        ],
        compiler_params=pltpu.CompilerParams(vmem_limit_bytes=16 * 1024 * 1024),
        name="finish",
    )(fold, *fields)
    return tuple(result)


def solution(mesh):
    level_rows_columns = P(None, "lat", "lon")
    return jax.shard_map(
        functools.partial(local, mesh.shape["lat"], mesh.shape["lon"]),
        mesh=mesh,
        in_specs=(
            level_rows_columns,
            level_rows_columns,
            level_rows_columns,
            level_rows_columns,
            P("lat", "lon"),
            P("lat", "lon"),
            level_rows_columns,
            level_rows_columns,
            P(),
        ),
        out_specs=(level_rows_columns,) * 2,
        check_vma=False,
    )
```

```python
import functools

import jax
import jax.numpy as jnp
from jax import lax
from jax.experimental import pallas as pl
from jax.experimental.pallas import tpu as pltpu
from jax.sharding import PartitionSpec as P

time_step = 0.2
scale = -time_step / 24.0
lanes = 128
group = 8
pad = 8
MESH = pl.DeviceIdType.MESH
f32 = jnp.float32


def chunk_count(levels, per):
    count = levels // per
    return next(c for c in (6, 3, 2, 1) if count % c == 0)


def roll(x, shift):
    return pltpu.roll(x, shift % lanes, 1)


def vroll(x, shift):
    return pltpu.roll(x, shift % group, 0)


def q(a, b, c, d):
    return 7.0 * (b + c) - (a + d)


def exchange_kernel(
    nlat, nlon, levels, rows,
    u_hbm, v_hbm, eu_hbm, ev_hbm, su_hbm, sv_hbm, mu_hbm, mv_hbm,
    u_part, v_part, low_own, high_own, keep, side, up_in, down_in, corner_u, corner_v, band,
    u_in, v_in, eu_in, ev_in, su_in, sv_in, mu_in, mv_in,
    edge_f, edge_m, um_n, vm_n, tv_n, cu_n, cv_n, um_t, vm_t, tu_t, ts_t,
    pack_own, pack_in, edge_own, edge_in, corner_u_own, corner_v_own, fix,
    edge_sem, load_sem, span_sem, up_send, up_recv, down_send, down_recv,
    lon_send, lon_recv, side_send, side_recv, diag_send, diag_recv, band_send, band_recv,
):
    per = lanes // rows
    tall = rows // group
    blocks = levels // per
    chunks = chunk_count(levels, per)
    depth = levels // chunks
    blocks_in = blocks // chunks
    groups = levels // group
    pitch = rows + pad
    step = next(n for n in (3, 2, 1) if blocks_in % n == 0)
    ahead = 2
    lat = lax.axis_index("lat")
    lon = lax.axis_index("lon")
    right = lax.rem(lon + 1, nlon)
    left = lax.rem(lon + nlon - 1, nlon)
    has_up = lat < nlat - 1
    has_down = lat > 0
    sides = 1 if nlon == 2 else 2
    picked = (0, 1, rows - 2, rows - 1)

    edges = [
        pltpu.make_async_copy(a.at[:, r, :], b.at[k, e], edge_sem.at[4 * s + e])
        for s, (a, b, k) in enumerate((
            (u_hbm, edge_f, 0), (mu_hbm, edge_m, 0), (v_hbm, edge_f, 1),
            (mv_hbm, edge_m, 1), (eu_hbm, edge_f, 2), (ev_hbm, edge_f, 3),
        ))
        for e, r in enumerate(picked)
    ]
    spans = [
        pltpu.make_async_copy(su_hbm, su_in, span_sem.at[0]),
        pltpu.make_async_copy(sv_hbm, sv_in, span_sem.at[1]),
    ]
    pairs = (
        (u_hbm, u_in), (mu_hbm, mu_in), (eu_hbm, eu_in),
        (v_hbm, v_in), (mv_hbm, mv_in), (ev_hbm, ev_in),
    )
    loads = [
        [
            pltpu.make_async_copy(
                a.at[pl.ds(c * depth, depth)], b.at[pl.ds(c * depth, depth)], load_sem.at[c, k]
            )
            for k, (a, b) in enumerate(pairs)
        ]
        for c in range(chunks)
    ]
    for copy in spans + edges:
        copy.start()

    def fetch(c):
        if c < chunks:
            for copy in loads[c]:
                copy.start()

    for c in range(ahead):
        fetch(c)

    barrier = pltpu.get_barrier_semaphore()

    def greet(where):
        pl.semaphore_signal(barrier, inc=1, device_id=where, device_id_type=MESH)

    greet((lat, right))
    if nlon > 2:
        greet((lat, left))

    @pl.when(has_up)
    def _():
        greet((lat + 1, lon))
        greet((lat + 1, left))

    @pl.when(has_down)
    def _():
        greet((lat - 1, lon))
        greet((lat - 1, right))

    if nlon > 3:
        @pl.when(lat == nlat - 1)
        def _():
            for d in range(2, nlon - 1):
                greet((lat, lax.rem(lon + d, nlon)))

    def arrive():
        @pl.when(lat == 0)
        def _():
            pl.semaphore_wait(barrier, sides + 2)

        @pl.when(has_up & has_down)
        def _():
            pl.semaphore_wait(barrier, sides + 4)

        @pl.when(lat == nlat - 1)
        def _():
            pl.semaphore_wait(barrier, sides + 2 + max(nlon - 3, 0))

    def remote(src, dst, send, recv, where):
        return pltpu.make_async_remote_copy(
            src_ref=src, dst_ref=dst, send_sem=send, recv_sem=recv,
            device_id=where, device_id_type=MESH,
        )

    def up_copy():
        return remote(high_own.at[pl.ds(0, 5)], up_in, up_send, up_recv, (lat + 1, lon))

    def down_copy():
        return remote(low_own, down_in, down_send, down_recv, (lat - 1, lon))

    def lon_copies(c):
        return [
            remote(
                pack_own.at[k, c], pack_in.at[k, c],
                lon_send.at[c, k], lon_recv.at[c, k], (lat, target),
            )
            for k, target in enumerate((right, left))
        ]

    def side_copies():
        return [
            remote(edge_own, edge_in.at[k], side_send.at[k], side_recv.at[k], (lat, target))
            for k, target in enumerate((right, left))
        ]

    def corner_down():
        return remote(
            corner_u_own, corner_u, diag_send.at[0], diag_recv.at[0], (lat - 1, right)
        )

    def corner_up():
        return remote(
            corner_v_own, corner_v, diag_send.at[1], diag_recv.at[1], (lat + 1, left)
        )

    def band_copy(d, k):
        return remote(
            high_own.at[k], band.at[lon, k], band_send.at[d, k], band_recv.at[d, k],
            (lat, lax.rem(lon + d, nlon)),
        )

    def band_arrival(d, k):
        origin = lax.rem(lon + nlon - d, nlon)
        return remote(
            high_own.at[k], band.at[origin, k], band_send.at[d, k], band_recv.at[d, k],
            (lat, lax.rem(lon + d, nlon)),
        )

    stages = chunks + 1

    def send_band(stage):
        @pl.when(lat == nlat - 1)
        def _():
            for k in range(6 * stage // stages, 6 * (stage + 1) // stages):
                for d in range(1, nlon):
                    band_copy(d, k).start()

    lane = lax.broadcasted_iota(jnp.int32, (group, lanes), 1)
    sub = lax.broadcasted_iota(jnp.int32, (group, lanes), 0)
    zero = jnp.zeros((group, lanes), f32)

    def clear(l, carry):
        for ref in (um_n, vm_n):
            ref[pl.ds(pl.multiple_of(l * pitch, group), group), :] = zero
        return carry

    lax.fori_loop(0, levels + 1, clear, 0)

    @pl.when(lat == 0)
    def _():
        up_in[...] = jnp.zeros((5, levels, lanes), f32)
        corner_v[...] = zero

    for copy in spans + edges:
        copy.wait()
    fetch(ahead)

    def edge_step(g, carry):
        part = pl.ds(pl.multiple_of(g * group, group), group)
        um, vm, tu, tv = [], [], [], []
        for e, r in enumerate(picked):
            mu = edge_m[0, e, part, :].astype(f32)
            mv = edge_m[1, e, part, :].astype(f32)
            um.append(mu * edge_f[0, e, part, :])
            vm.append(mv * edge_f[1, e, part, :])
            vol_u = su_in[pl.ds(r, 1), :] * edge_f[2, e, part, :]
            vol_v = sv_in[pl.ds(r, 1), :] * edge_f[3, e, part, :]
            tu.append(vol_u * um[e])
            tv.append(vol_v * vm[e])
            keep[e, part, :] = mu * scale / vol_u
            keep[4 + e, part, :] = mv * scale / vol_v
        for k, x in enumerate((um[0], um[1], vm[0], vm[1], tu[0], tv[0])):
            low_own[k, part, :] = x
        for k, x in enumerate((um[2], um[3], vm[2], vm[3], tv[3], tu[3])):
            high_own[k, part, :] = x
            band[lon, k, part, :] = x
        keep[8, part, :] = tv[1]
        keep[9, part, :] = tv[2]
        return carry

    lax.fori_loop(0, groups, edge_step, 0)
    arrive()

    @pl.when(has_down)
    def _():
        down_copy().start()

    @pl.when(has_up)
    def _():
        up_copy().start()

    send_band(0)

    first, second, ring = zero, zero, zero
    for g in range(groups):
        part = pl.ds(g * group, group)
        first = jnp.where(lane == g, roll(low_own[4, part, :], g + 1), first)
        tv_top = high_own[4, part, :]
        second = jnp.where(lane == g, roll(tv_top, g), second)
        ring = jnp.where(lane // 4 == g, roll(high_own[3, part, :], 4 * g + 2), ring)
        for k, x in enumerate((low_own[5, part, :], keep[9, part, :], tv_top)):
            ring = jnp.where(lane == 64 + 4 * g + k, roll(x, 64 + 4 * g + k), ring)
    corner_u_own[...] = first
    corner_v_own[...] = second
    edge_own[...] = ring
    for copy in side_copies():
        copy.start()

    @pl.when(has_down)
    def _():
        corner_down().start()

    @pl.when(has_up)
    def _():
        corner_up().start()

    def prepare(block, c):
        um_b, vm_b, tu_b, ts_b, tv_b = [], [], [], [], []
        for s in range(per):
            l = block * per + s
            base = pl.multiple_of(l * pitch + pad, group)
            tus = []
            for b in range(tall):
                at = pl.ds(b * group, group)
                mu = mu_in[l, at, :].astype(f32)
                mv = mv_in[l, at, :].astype(f32)
                um = mu * u_in[l, at, :]
                vm = mv * v_in[l, at, :]
                vol_u = su_in[at, :] * eu_in[l, at, :]
                vol_v = sv_in[at, :] * ev_in[l, at, :]
                tv = vol_v * vm
                tus.append(vol_u * um)
                um_n[pl.ds(base + b * group, group), :] = um
                vm_n[pl.ds(base + b * group, group), :] = vm
                tv_n[l, at, :] = tv
                cu_n[l, at, :] = mu * scale / vol_u
                cv_n[l, at, :] = mv * scale / vol_v
                um_b.append(um)
                vm_b.append(vm)
                tv_b.append(tv)
            turned = [vroll(x, -1) for x in tus] + [zero]
            for b in range(tall):
                ts_b.append(tus[b] + jnp.where(sub == group - 1, turned[b + 1], turned[b]))
            tu_b += tus
        here = block - c * blocks_in
        own = pl.ds(here, 1)

        def flip(tiles):
            return jnp.concatenate(tiles, axis=0).T

        for x, ref, west, east in (
            (flip(um_b), um_t, 0, 0), (flip(vm_b), vm_t, 2, 2),
        ):
            ref[block, pl.ds(pad, lanes), :] = x
            for k in range(2):
                pack_own[0, c, west + k, own, :] = x[lanes - 2 + k:lanes - 1 + k]
                pack_own[1, c, east + k, own, :] = x[k:k + 1]
        x = flip(tu_b)
        tu_t[block, pl.ds(pad, lanes), :] = x
        pack_own[0, c, 4, own, :] = x[lanes - 1:]
        pack_own[1, c, 4, own, :] = x[:1]
        x = flip(ts_b)
        ts_t[block, pl.ds(pad, lanes), :] = x
        pack_own[0, c, 5, own, :] = x[lanes - 1:]
        pack_own[1, c, 5, own, :] = flip(tv_b)[:1]
        inside(block)

    def inside(block):
        for s in range(per):
            l = block * per + s
            base = l * pitch + pad

            def um(b, shift):
                return um_n[pl.ds(base + b * group + shift, group), :]

            def vm(b, shift):
                return vm_n[pl.ds(base + b * group + shift, group), :]

            f, w, tv_turned = [], [], []
            for b in range(tall):
                at = pl.ds(b * group, group)
                tv = tv_n[l, at, :]
                tv_turned.append(vroll(tv, 1))
                below = jnp.where(sub == 0, tv_turned[b - 1] if b else zero, tv_turned[b])
                f.append((tv + roll(tv, -1)) * q(um(b, -1), um(b, 0), um(b, 1), um(b, 2)))
                cross = (below + tv) * q(vm(b, -2), vm(b, -1), vm(b, 0), vm(b, 1))
                w.append(jnp.where(sub == 0, 0.0, cross) if b == 0 else cross)
            f_turned = [vroll(x, 1) for x in f]
            w_turned = [vroll(x, -1) for x in w] + [zero]
            for b in range(tall):
                at = pl.ds(b * group, group)
                below = jnp.where(sub == 0, f_turned[b - 1] if b else zero, f_turned[b])
                above = jnp.where(sub == group - 1, w_turned[b + 1], w_turned[b])
                u_part[l, at, :] = um(b, 0) + cu_n[l, at, :] * (f[b] - below)
                v_part[l, at, :] = vm(b, 0) + cv_n[l, at, :] * (above - w[b])

    slot = lax.broadcasted_iota(jnp.int32, (blocks_in, lanes), 1) % rows

    def lane_fix(c):
        own = pack_own[0, c, 1]

        def shifted(x, by):
            keep_it = (slot + by >= 0) & (slot + by < rows)
            return jnp.where(keep_it, pltpu.roll(x, (-by) % lanes, 1), 0.0)

        flux = (pack_in[1, c, 5] - pack_own[1, c, 5]) * q(
            shifted(own, -1), own, shifted(own, 1), shifted(own, 2)
        )
        fix[c] = flux - shifted(flux, -1)

    def across(block, c):
        here = pl.ds(block - c * blocks_in, 1)
        for ref, at in ((um_t, 0), (vm_t, 2)):
            for k in range(2):
                ref[block, pl.ds(pad - 2 + k, 1), :] = pack_in[0, c, at + k, here, :]
                ref[block, pl.ds(pad + lanes + k, 1), :] = pack_in[1, c, at + k, here, :]
        tu_t[block, pl.ds(pad - 1, 1), :] = pack_in[0, c, 4, here, :]
        tu_t[block, pl.ds(pad + lanes, 1), :] = pack_in[1, c, 4, here, :]
        ts_t[block, pl.ds(pad - 1, 1), :] = pack_in[0, c, 5, here, :]

        def read(ref, i):
            return ref[block, pl.ds(pad + i, group), :]

        def west(i):
            return (read(tu_t, i - 1) + read(tu_t, i)) * q(*[read(um_t, i + k) for k in (-2, -1, 0, 1)])

        def east(i):
            return read(ts_t, i) * q(*[read(vm_t, i + k) for k in (-1, 0, 1, 2)])

        count = lanes // group
        fs = [west(i * group) for i in range(count)]
        gs = [east(i * group) for i in range(count)]
        f_turned = [vroll(x, -1) for x in fs] + [west(lanes - group + 1)]
        g_turned = [east(-1)] + [vroll(x, 1) for x in gs]
        du = [
            jnp.where(sub == group - 1, f_turned[i + 1], f_turned[i]) - fs[i] for i in range(count)
        ]
        dv = [gs[i] - jnp.where(sub == 0, g_turned[i], g_turned[i + 1]) for i in range(count)]
        du[-1] = du[-1] + jnp.where(sub == group - 1, fix[c, here, :], 0.0)
        du = jnp.concatenate(du, axis=0).T
        dv = jnp.concatenate(dv, axis=0).T
        for s in range(per):
            l = block * per + s
            for b in range(tall):
                at = pl.ds(b * group, group)
                k = (s * tall + b) * group
                u_part[l, at, :] = u_part[l, at, :] + cu_n[l, at, :] * du[k:k + group]
                v_part[l, at, :] = v_part[l, at, :] + cv_n[l, at, :] * dv[k:k + group]

    def every(body, c):
        def run(i, carry):
            for k in range(step):
                body(i * step + k)
            return carry

        lax.fori_loop(c * blocks_in // step, (c + 1) * blocks_in // step, run, 0)

    for c in range(chunks):
        for copy in loads[c]:
            copy.wait()
        fetch(c + ahead + 1)
        every(lambda i: prepare(i, c), c)
        for copy in lon_copies(c):
            copy.start()
        send_band(c + 1)

    for copy in side_copies():
        copy.wait()
    for g in range(groups):
        part = pl.ds(g * group, group)
        from_left, from_right = edge_in[0], edge_in[1]
        for k, x in enumerate((low_own[5, part, :], keep[9, part, :], high_own[4, part, :])):
            halo = roll(from_right, -(64 + 4 * g + k))
            side[k, part, :] = x + roll(jnp.where(lane == 0, halo, x), -1)
        vm = high_own[3, part, :]
        halo = roll(jnp.where(lane % 4 < 2, from_left, from_right), -(4 * g + 2))
        w2 = roll(jnp.where(lane >= lanes - 2, halo, vm), 2)
        w1 = roll(jnp.where(lane == lanes - 1, halo, vm), 1)
        e1 = roll(jnp.where(lane == 0, halo, vm), -1)
        e2 = roll(jnp.where(lane < 2, halo, vm), -2)
        side[3, part, :] = q(w2, w1, vm, e1)
        side[4, part, :] = q(w1, vm, e1, e2)

    for c in range(chunks):
        for copy in lon_copies(c):
            copy.wait()
        lane_fix(c)
        every(lambda i: across(i, c), c)

    @pl.when(has_down)
    def _():
        down_copy().wait_send()
        corner_down().wait_send()
        up_copy().wait_recv()
        corner_up().wait_recv()

    @pl.when(has_up)
    def _():
        up_copy().wait_send()
        corner_up().wait_send()
        down_copy().wait_recv()
        corner_down().wait_recv()

    @pl.when(lat == nlat - 1)
    def _():
        for d in range(1, nlon):
            for k in range(6):
                band_copy(d, k).wait_send()
                band_arrival(d, k).wait_recv()


def finish_kernel(
    nlat, nlon, levels, rows,
    fold_ref, u_part, v_part, low_own, high_own, keep, side, up_in, down_in, corner_u, corner_v, band,
    u_out, v_out,
    high, high_left, u_low, u_high, v_low, v_high, sem,
):
    lat = lax.axis_index("lat")
    lon = lax.axis_index("lon")
    groups = levels // group
    width = nlon * lanes
    lane = lax.broadcasted_iota(jnp.int32, (group, lanes), 1)
    middle = pl.ds(group, rows - 2 * group)
    low = pl.ds(0, group)
    top = pl.ds(rows - group, group)
    first = [
        pltpu.make_async_copy(a.at[:, middle], b.at[:, middle], sem.at[k])
        for k, (a, b) in enumerate(((u_part, u_out), (v_part, v_out)))
    ]
    for copy in first:
        copy.start()

    @pl.when(lat == nlat - 1)
    def _():
        start = fold_ref[0]
        own = lax.rem(start - lon * lanes - lane + 2 * width, width)
        before = jnp.zeros_like(lane) + lax.rem(start - lon * lanes + 1 + 2 * width, width)

        def pick(k, part, index):
            block = index // lanes
            spot = index % lanes
            got = jnp.zeros((group, lanes), f32)
            for b in range(nlon):
                taken = jnp.take_along_axis(
                    band[b, k, part, :], spot, axis=1, mode="promise_in_bounds"
                )
                got = jnp.where(block == b, taken, got)
            return -got

        for g in range(groups):
            part = pl.ds(g * group, group)
            for k, source in enumerate((1, 0, 3, 2, 5, 4)):
                high[k, part, :] = pick(source, part, own)
            high_left[part, :] = pick(5, part, before)

    @pl.when(lat < nlat - 1)
    def _():
        for g in range(groups):
            part = pl.ds(g * group, group)
            for k in range(6):
                high[k, part, :] = down_in[k, part, :]
            high_left[part, :] = roll(corner_u[...], lanes - 1 - g)

    def copy_tiles(l, carry):
        for source, a, b in ((u_part, u_low, u_high), (v_part, v_low, v_high)):
            a[l] = source[l, low, :]
            b[l] = source[l, top, :]
        return carry

    lax.fori_loop(0, levels, copy_tiles, 0, unroll=8)

    views = [ref.reshape(levels * group, lanes) for ref in (u_low, u_high, v_low, v_high)]

    def add(view, g, row, value):
        at = pl.ds(g * group * group + row, group, stride=group)
        view[at, :] = view[at, :] + value

    for g in range(groups):
        part = pl.ds(g * group, group)
        um0, um1, vm0, vm1, _, tv0 = [low_own[k, part, :] for k in range(6)]
        vm30, vm31, tv31 = [high_own[k, part, :] for k in (2, 3, 4)]
        um_2, um_1, vm_2, vm_1, tv_1 = [up_in[k, part, :] for k in range(5)]
        um32, um33, vm32, vm33, tu32, tv32 = [high[k, part, :] for k in range(6)]
        cu0, cu1, cu30, cu31, cv0, cv1, cv30, cv31, tv1, tv30 = [keep[k, part, :] for k in range(10)]
        v0, v30, v31, q_west, q_east = [side[k, part, :] for k in range(5)]

        face = tv_1 + roll(jnp.where(lane == 0, roll(corner_v[...], -g), tv_1), -1)
        f_low = face * q(um_2, um_1, um0, um1)
        d0 = v0 * um_1
        add(views[0], g, 0, -cu0 * (d0 + f_low))
        add(views[0], g, 1, cu1 * d0)
        w_low = (tv_1 + tv0) * q(vm_2, vm_1, vm0, vm1)
        d0 = (tv0 + tv1) * vm_1
        add(views[2], g, 0, -cv0 * (d0 + w_low))
        add(views[2], g, 1, cv1 * d0)
        d30 = v30 * um32
        add(views[1], g, group - 2, -cu30 * d30)
        add(views[1], g, group - 1, cu31 * (v31 * (7.0 * um32 - um33) + d30))
        d30 = (tv30 + tv31) * vm32
        w_high = (tv31 + tv32) * q(vm30, vm31, vm32, vm33)
        tu_west = roll(jnp.where(lane == lanes - 1, high_left[part, :], tu32), 1)
        add(views[3], g, group - 2, -cv30 * d30)
        add(views[3], g, group - 1, cv31 * (w_high + d30 + (tu32 * q_east - tu_west * q_west)))

    last = [
        pltpu.make_async_copy(a, b.at[:, at], sem.at[2 + k])
        for k, (a, b, at) in enumerate((
            (u_low, u_out, low), (u_high, u_out, top), (v_low, v_out, low), (v_high, v_out, top),
        ))
    ]
    for copy in last:
        copy.start()
    for copy in first + last:
        copy.wait()


def local(nlat, nlon, u, v, eu, ev, su, sv, mu, mv, fold):
    u, v, eu, ev, su, sv, mu, mv = [
        pltpu.with_memory_space_constraint(x, pltpu.HBM) for x in (u, v, eu, ev, su, sv, mu, mv)
    ]
    levels, rows, _ = u.shape
    per = lanes // rows
    blocks = levels // per
    chunks = chunk_count(levels, per)
    blocks_in = blocks // chunks
    pitch = rows + pad
    vmem = pl.BlockSpec(memory_space=pltpu.VMEM)
    hbm = pl.BlockSpec(memory_space=pltpu.HBM)
    block = (levels, rows, lanes)
    line = (levels, lanes)
    shapes = [
        block, block,
        (6,) + line, (6,) + line, (10,) + line, (5,) + line, (5,) + line, (6,) + line,
        (group, lanes), (group, lanes), (nlon, 6) + line,
    ]
    tall = (levels * pitch + pad, lanes)
    turned = (blocks, lanes + 2 * pad, lanes)
    packs = (2, chunks, 6, blocks_in, lanes)
    dma = pltpu.SemaphoreType.DMA
    V = pltpu.VMEM
    fields = pl.pallas_call(
        functools.partial(exchange_kernel, nlat, nlon, levels, rows),
        out_shape=[V(s, f32) for s in shapes],
        in_specs=[hbm] * 8,
        out_specs=[vmem] * len(shapes),
        scratch_shapes=[
            V(block, f32), V(block, f32), V(block, f32), V(block, f32),
            V((rows, lanes), f32), V((rows, lanes), f32),
            V(block, jnp.int32), V(block, jnp.int32),
            V((4, 4) + line, f32), V((2, 4) + line, jnp.int32),
            V(tall, f32), V(tall, f32), V(block, f32), V(block, f32), V(block, f32),
            V(turned, f32), V(turned, f32), V(turned, f32), V(turned, f32),
            V(packs, f32), V(packs, f32),
            V((group, lanes), f32), V((2, group, lanes), f32),
            V((group, lanes), f32), V((group, lanes), f32),
            V((chunks, blocks_in, lanes), f32),
            dma((24,)), dma((chunks, 6)), dma((2,)),
            dma, dma, dma, dma,
            dma((chunks, 2)), dma((chunks, 2)), dma((2,)), dma((2,)), dma((2,)), dma((2,)),
            dma((nlon, 6)), dma((nlon, 6)),
        ],
        compiler_params=pltpu.CompilerParams(
            collective_id=0, has_side_effects=True, vmem_limit_bytes=36 * 1024 * 1024
        ),
        name="exchange",
    )(u, v, eu, ev, su, sv, mu, mv)
    strip = (levels, group, lanes)
    result = pl.pallas_call(
        functools.partial(finish_kernel, nlat, nlon, levels, rows),
        out_shape=[jax.ShapeDtypeStruct(block, f32)] * 2,
        in_specs=[pl.BlockSpec(memory_space=pltpu.SMEM)] + [vmem] * len(shapes),
        out_specs=[hbm] * 2,
        scratch_shapes=[
            V((6,) + line, f32), V(line, f32),
            V(strip, f32), V(strip, f32), V(strip, f32), V(strip, f32),
            dma((6,)),
        ],
        compiler_params=pltpu.CompilerParams(vmem_limit_bytes=16 * 1024 * 1024),
        name="finish",
    )(fold, *fields)
    return tuple(result)


def solution(mesh):
    level_rows_columns = P(None, "lat", "lon")
    return jax.shard_map(
        functools.partial(local, mesh.shape["lat"], mesh.shape["lon"]),
        mesh=mesh,
        in_specs=(
            level_rows_columns,
            level_rows_columns,
            level_rows_columns,
            level_rows_columns,
            P("lat", "lon"),
            P("lat", "lon"),
            level_rows_columns,
            level_rows_columns,
            P(),
        ),
        out_specs=(level_rows_columns,) * 2,
        check_vma=False,
    )
```

```python
import functools

import jax
import jax.numpy as jnp
from jax import lax
from jax.experimental import pallas as pl
from jax.experimental.pallas import tpu as pltpu
from jax.sharding import PartitionSpec as P

time_step = 0.2
scale = -time_step / 24.0
lanes = 128
group = 8
pad = 8
MESH = pl.DeviceIdType.MESH
f32 = jnp.float32


def chunk_count(levels, per):
    count = levels // per
    return next(c for c in (6, 3, 2, 1) if count % c == 0)


def roll(x, shift):
    return pltpu.roll(x, shift % lanes, 1)


def vroll(x, shift):
    return pltpu.roll(x, shift % group, 0)


def q(a, b, c, d):
    return 7.0 * (b + c) - (a + d)


def exchange_kernel(
    nlat, nlon, levels, rows,
    u_hbm, v_hbm, eu_hbm, ev_hbm, su_hbm, sv_hbm, mu_hbm, mv_hbm,
    u_part, v_part, low_own, high_own, keep, side, up_in, down_in, corner_u, corner_v, band,
    real_in, mask_in, span_in,
    edge_f, edge_m, um_n, vm_n, tv_n, cu_n, cv_n, um_t, vm_t, tu_t, ts_t,
    pack_own, pack_in, edge_own, edge_in, fix,
    early_sem, load_sem, up_send, up_recv, down_send, down_recv,
    lon_send, lon_recv, side_send, side_recv, diag_send, diag_recv, band_send, band_recv,
):
    per = lanes // rows
    tall = rows // group
    blocks = levels // per
    chunks = chunk_count(levels, per)
    blocks_in = blocks // chunks
    groups = levels // group
    pitch = rows + pad
    step = next(n for n in (3, 2, 1) if blocks_in % n == 0)
    loads = 3 if chunks % 3 == 0 else chunks
    depth = levels // loads
    lat = lax.axis_index("lat")
    lon = lax.axis_index("lon")
    right = lax.rem(lon + 1, nlon)
    left = lax.rem(lon + nlon - 1, nlon)
    has_up = lat < nlat - 1
    has_down = lat > 0
    targets = (right,) if nlon == 2 else (right, left)
    sides = len(targets)
    picked = (0, 1, rows - 2, rows - 1)

    reals = (u_hbm, v_hbm, eu_hbm, ev_hbm)
    masks = (mu_hbm, mv_hbm)

    def fetch_edges(sources, edge, sem):
        for k, source in enumerate(sources):
            for e, r in enumerate(picked):
                pltpu.make_async_copy(source.at[:, r, :], edge.at[k, e], sem).start()

    def fetch_part(c):
        part = pl.ds(c * depth, depth)
        for k, source in enumerate(reals):
            pltpu.make_async_copy(source.at[part], real_in.at[k, part], load_sem.at[c, 0]).start(priority=1)
        for k, source in enumerate(masks):
            pltpu.make_async_copy(source.at[part], mask_in.at[k, part], load_sem.at[c, 1]).start(priority=1)

    def landed(ref, sem):
        pltpu.make_async_copy(ref, ref, sem).wait()

    fetch_edges(reals, edge_f, early_sem.at[0])
    fetch_edges(masks, edge_m, early_sem.at[1])
    pltpu.make_async_copy(su_hbm, span_in.at[0], early_sem.at[2]).start()
    pltpu.make_async_copy(sv_hbm, span_in.at[1], early_sem.at[2]).start()
    for c in range(loads):
        fetch_part(c)

    barrier = pltpu.get_barrier_semaphore()

    def greet(where):
        pl.semaphore_signal(barrier, inc=1, device_id=where, device_id_type=MESH)

    greet((lat, right))
    if nlon > 2:
        greet((lat, left))

    @pl.when(has_up)
    def _():
        greet((lat + 1, lon))

    @pl.when(has_down)
    def _():
        greet((lat - 1, lon))

    if nlon > 3:
        @pl.when(lat == nlat - 1)
        def _():
            for d in range(2, nlon - 1):
                greet((lat, lax.rem(lon + d, nlon)))

    def arrive():
        @pl.when(lat == 0)
        def _():
            pl.semaphore_wait(barrier, sides + 1)

        @pl.when(has_up & has_down)
        def _():
            pl.semaphore_wait(barrier, sides + 2)

        @pl.when(lat == nlat - 1)
        def _():
            pl.semaphore_wait(barrier, sides + 1 + max(nlon - 3, 0))

    def remote(src, dst, send, recv, where):
        return pltpu.make_async_remote_copy(
            src_ref=src, dst_ref=dst, send_sem=send, recv_sem=recv,
            device_id=where, device_id_type=MESH,
        )

    def up_copy():
        return remote(high_own.at[pl.ds(0, 5)], up_in, up_send, up_recv, (lat + 1, lon))

    def down_copy():
        return remote(low_own, down_in, down_send, down_recv, (lat - 1, lon))

    def lon_copies(c):
        if nlon == 2:
            return [remote(pack_own.at[:, c], pack_in.at[:, c], lon_send.at[0], lon_recv.at[c, 0], (lat, right))]
        return [
            remote(pack_own.at[k, c], pack_in.at[k, c], lon_send.at[k], lon_recv.at[c, k], (lat, target))
            for k, target in enumerate(targets)
        ]

    def lon_sent():
        if nlon == 2:
            return [remote(pack_own, pack_in, lon_send.at[0], lon_recv.at[0, 0], (lat, right))]
        return [
            remote(pack_own.at[k], pack_in.at[k], lon_send.at[k], lon_recv.at[0, k], (lat, target))
            for k, target in enumerate(targets)
        ]

    def side_copies():
        return [
            remote(edge_own, edge_in.at[k], side_send.at[k], side_recv.at[k], (lat, target))
            for k, target in enumerate(targets)
        ]

    def corner_down():
        return remote(edge_in.at[0], corner_u, diag_send.at[0], diag_recv.at[0], (lat - 1, lon))

    def corner_up():
        return remote(edge_in.at[sides - 1], corner_v, diag_send.at[1], diag_recv.at[1], (lat + 1, lon))

    def band_copy(d, k):
        return remote(
            high_own.at[k], band.at[lon, k], band_send.at[d], band_recv.at[d],
            (lat, lax.rem(lon + d, nlon)),
        )

    def band_sent(d):
        return remote(
            high_own, band.at[lon], band_send.at[d], band_recv.at[d],
            (lat, lax.rem(lon + d, nlon)),
        )

    def band_arrival(d):
        origin = lax.rem(lon + nlon - d, nlon)
        return remote(
            high_own, band.at[origin], band_send.at[d], band_recv.at[d],
            (lat, lax.rem(lon + d, nlon)),
        )

    stages = chunks + 1

    def send_band(stage):
        @pl.when(lat == nlat - 1)
        def _():
            for k in range(6 * stage // stages, 6 * (stage + 1) // stages):
                for d in range(1, nlon):
                    band_copy(d, k).start()

    lane = lax.broadcasted_iota(jnp.int32, (group, lanes), 1)
    sub = lax.broadcasted_iota(jnp.int32, (group, lanes), 0)
    zero = jnp.zeros((group, lanes), f32)

    def clear(l, carry):
        for ref in (um_n, vm_n):
            ref[pl.ds(pl.multiple_of(l * pitch, group), group), :] = zero
        return carry

    lax.fori_loop(0, levels + 1, clear, 0)

    @pl.when(lat == 0)
    def _():
        up_in[...] = jnp.zeros((5, levels, lanes), f32)
        corner_v[...] = zero

    landed(edge_f, early_sem.at[0])
    landed(edge_m, early_sem.at[1])
    landed(span_in, early_sem.at[2])

    def edge_step(g, carry):
        part = pl.ds(pl.multiple_of(g * group, group), group)
        um, vm, tu, tv = [], [], [], []
        for e, r in enumerate(picked):
            mu = edge_m[0, e, part, :].astype(f32)
            mv = edge_m[1, e, part, :].astype(f32)
            um.append(mu * edge_f[0, e, part, :])
            vm.append(mv * edge_f[1, e, part, :])
            vol_u = span_in[0, pl.ds(r, 1), :] * edge_f[2, e, part, :]
            vol_v = span_in[1, pl.ds(r, 1), :] * edge_f[3, e, part, :]
            tu.append(vol_u * um[e])
            tv.append(vol_v * vm[e])
            keep[e, part, :] = mu * scale / vol_u
            keep[4 + e, part, :] = mv * scale / vol_v
        for k, x in enumerate((um[0], um[1], vm[0], vm[1], tu[0], tv[0])):
            low_own[k, part, :] = x
        for k, x in enumerate((um[2], um[3], vm[2], vm[3], tv[3], tu[3])):
            high_own[k, part, :] = x
            band[lon, k, part, :] = x
        keep[8, part, :] = tv[1]
        keep[9, part, :] = tv[2]
        return carry

    lax.fori_loop(0, groups, edge_step, 0)
    arrive()

    @pl.when(has_down)
    def _():
        down_copy().start()

    @pl.when(has_up)
    def _():
        up_copy().start()

    send_band(0)

    ring = zero
    for g in range(groups):
        part = pl.ds(g * group, group)
        tv_top = high_own[4, part, :]
        ring = jnp.where(lane // 4 == g, roll(high_own[3, part, :], 4 * g + 2), ring)
        for k, x in enumerate((low_own[5, part, :], keep[9, part, :], tv_top)):
            ring = jnp.where(lane == 64 + 4 * g + k, roll(x, 64 + 4 * g + k), ring)
        ring = jnp.where(lane == 64 + 4 * g + 3, roll(low_own[4, part, :], 64 + 4 * g + 4), ring)
    edge_own[...] = ring
    for copy in side_copies():
        copy.start()

    def prepare(block, c):
        um_b, vm_b, tu_b, ts_b, tv_b = [], [], [], [], []
        for s in range(per):
            l = block * per + s
            base = pl.multiple_of(l * pitch + pad, group)
            tus = []
            for b in range(tall):
                at = pl.ds(b * group, group)
                mu = mask_in[0, l, at, :].astype(f32)
                mv = mask_in[1, l, at, :].astype(f32)
                um = mu * real_in[0, l, at, :]
                vm = mv * real_in[1, l, at, :]
                vol_u = span_in[0, at, :] * real_in[2, l, at, :]
                vol_v = span_in[1, at, :] * real_in[3, l, at, :]
                tv = vol_v * vm
                tus.append(vol_u * um)
                um_n[pl.ds(base + b * group, group), :] = um
                vm_n[pl.ds(base + b * group, group), :] = vm
                tv_n[l, at, :] = tv
                cu_n[l, at, :] = mu * scale / vol_u
                cv_n[l, at, :] = mv * scale / vol_v
                um_b.append(um)
                vm_b.append(vm)
                tv_b.append(tv)
            turned = [vroll(x, -1) for x in tus] + [zero]
            for b in range(tall):
                ts_b.append(tus[b] + jnp.where(sub == group - 1, turned[b + 1], turned[b]))
            tu_b += tus
        here = block - c * blocks_in
        own = pl.ds(here, 1)

        def flip(tiles):
            return jnp.concatenate(tiles, axis=0).T

        for x, ref, west, east in (
            (flip(um_b), um_t, 0, 0), (flip(vm_b), vm_t, 2, 2),
        ):
            ref[block, pl.ds(pad, lanes), :] = x
            for k in range(2):
                pack_own[0, c, west + k, own, :] = x[lanes - 2 + k:lanes - 1 + k]
                pack_own[1, c, east + k, own, :] = x[k:k + 1]
        x = flip(tu_b)
        tu_t[block, pl.ds(pad, lanes), :] = x
        pack_own[0, c, 4, own, :] = x[lanes - 1:]
        pack_own[1, c, 4, own, :] = x[:1]
        x = flip(ts_b)
        ts_t[block, pl.ds(pad, lanes), :] = x
        pack_own[0, c, 5, own, :] = x[lanes - 1:]
        pack_own[1, c, 5, own, :] = flip(tv_b)[:1]
        inside(block)

    def inside(block):
        for s in range(per):
            l = block * per + s
            base = l * pitch + pad

            def um(b, shift):
                return um_n[pl.ds(base + b * group + shift, group), :]

            def vm(b, shift):
                return vm_n[pl.ds(base + b * group + shift, group), :]

            f, w, tv_turned = [], [], []
            for b in range(tall):
                at = pl.ds(b * group, group)
                tv = tv_n[l, at, :]
                tv_turned.append(vroll(tv, 1))
                below = jnp.where(sub == 0, tv_turned[b - 1] if b else zero, tv_turned[b])
                f.append((tv + roll(tv, -1)) * q(um(b, -1), um(b, 0), um(b, 1), um(b, 2)))
                cross = (below + tv) * q(vm(b, -2), vm(b, -1), vm(b, 0), vm(b, 1))
                w.append(jnp.where(sub == 0, 0.0, cross) if b == 0 else cross)
            f_turned = [vroll(x, 1) for x in f]
            w_turned = [vroll(x, -1) for x in w] + [zero]
            for b in range(tall):
                at = pl.ds(b * group, group)
                below = jnp.where(sub == 0, f_turned[b - 1] if b else zero, f_turned[b])
                above = jnp.where(sub == group - 1, w_turned[b + 1], w_turned[b])
                u_part[l, at, :] = um(b, 0) + cu_n[l, at, :] * (f[b] - below)
                v_part[l, at, :] = vm(b, 0) + cv_n[l, at, :] * (above - w[b])

    slot = lax.broadcasted_iota(jnp.int32, (blocks_in, lanes), 1) % rows

    def lane_fix(c):
        own = pack_own[0, c, 1]

        def shifted(x, by):
            keep_it = (slot + by >= 0) & (slot + by < rows)
            return jnp.where(keep_it, pltpu.roll(x, (-by) % lanes, 1), 0.0)

        flux = (pack_in[1, c, 5] - pack_own[1, c, 5]) * q(
            shifted(own, -1), own, shifted(own, 1), shifted(own, 2)
        )
        fix[c] = flux - shifted(flux, -1)

    def across(block, c):
        here = pl.ds(block - c * blocks_in, 1)
        for ref, at in ((um_t, 0), (vm_t, 2)):
            for k in range(2):
                ref[block, pl.ds(pad - 2 + k, 1), :] = pack_in[0, c, at + k, here, :]
                ref[block, pl.ds(pad + lanes + k, 1), :] = pack_in[1, c, at + k, here, :]
        tu_t[block, pl.ds(pad - 1, 1), :] = pack_in[0, c, 4, here, :]
        tu_t[block, pl.ds(pad + lanes, 1), :] = pack_in[1, c, 4, here, :]
        ts_t[block, pl.ds(pad - 1, 1), :] = pack_in[0, c, 5, here, :]

        def read(ref, i):
            return ref[block, pl.ds(pad + i, group), :]

        def west(i):
            return (read(tu_t, i - 1) + read(tu_t, i)) * q(*[read(um_t, i + k) for k in (-2, -1, 0, 1)])

        def east(i):
            return read(ts_t, i) * q(*[read(vm_t, i + k) for k in (-1, 0, 1, 2)])

        count = lanes // group
        fs = [west(i * group) for i in range(count)]
        gs = [east(i * group) for i in range(count)]
        f_turned = [vroll(x, -1) for x in fs] + [west(lanes - group + 1)]
        g_turned = [east(-1)] + [vroll(x, 1) for x in gs]
        du = [
            jnp.where(sub == group - 1, f_turned[i + 1], f_turned[i]) - fs[i] for i in range(count)
        ]
        dv = [gs[i] - jnp.where(sub == 0, g_turned[i], g_turned[i + 1]) for i in range(count)]
        du[-1] = du[-1] + jnp.where(sub == group - 1, fix[c, here, :], 0.0)
        du = jnp.concatenate(du, axis=0).T
        dv = jnp.concatenate(dv, axis=0).T
        for s in range(per):
            l = block * per + s
            for b in range(tall):
                at = pl.ds(b * group, group)
                k = (s * tall + b) * group
                u_part[l, at, :] = u_part[l, at, :] + cu_n[l, at, :] * du[k:k + group]
                v_part[l, at, :] = v_part[l, at, :] + cv_n[l, at, :] * dv[k:k + group]

    def every(body, c):
        def run(i, carry):
            for k in range(step):
                body(i * step + k)
            return carry

        lax.fori_loop(c * blocks_in // step, (c + 1) * blocks_in // step, run, 0)

    for c in range(chunks):
        if c * loads % chunks == 0:
            part = pl.ds(c * loads // chunks * depth, depth)
            landed(real_in.at[:, part], load_sem.at[c * loads // chunks, 0])
            landed(mask_in.at[:, part], load_sem.at[c * loads // chunks, 1])
        every(lambda i: prepare(i, c), c)
        for copy in lon_copies(c):
            copy.start()
        send_band(c + 1)

    for copy in side_copies():
        copy.wait()

    @pl.when(has_down)
    def _():
        corner_down().start()

    @pl.when(has_up)
    def _():
        corner_up().start()

    for g in range(groups):
        part = pl.ds(g * group, group)
        from_left, from_right = edge_in[0], edge_in[sides - 1]
        for k, x in enumerate((low_own[5, part, :], keep[9, part, :], high_own[4, part, :])):
            halo = roll(from_right, -(64 + 4 * g + k))
            side[k, part, :] = x + roll(jnp.where(lane == 0, halo, x), -1)
        vm = high_own[3, part, :]
        halo = roll(jnp.where(lane % 4 < 2, from_left, from_right), -(4 * g + 2))
        w2 = roll(jnp.where(lane >= lanes - 2, halo, vm), 2)
        w1 = roll(jnp.where(lane == lanes - 1, halo, vm), 1)
        e1 = roll(jnp.where(lane == 0, halo, vm), -1)
        e2 = roll(jnp.where(lane < 2, halo, vm), -2)
        side[3, part, :] = q(w2, w1, vm, e1)
        side[4, part, :] = q(w1, vm, e1, e2)

    for c in range(chunks):
        for copy in lon_copies(c):
            copy.wait_recv()
        lane_fix(c)
        every(lambda i: across(i, c), c)

    for copy in lon_sent():
        copy.wait_send()

    @pl.when(has_down)
    def _():
        down_copy().wait_send()
        corner_down().wait_send()
        up_copy().wait_recv()
        corner_up().wait_recv()

    @pl.when(has_up)
    def _():
        up_copy().wait_send()
        corner_up().wait_send()
        down_copy().wait_recv()
        corner_down().wait_recv()

    @pl.when(lat == nlat - 1)
    def _():
        for d in range(1, nlon):
            band_sent(d).wait_send()
            band_arrival(d).wait_recv()


def finish_kernel(
    nlat, nlon, levels, rows,
    fold_ref, u_part, v_part, low_own, high_own, keep, side, up_in, down_in, corner_u, corner_v, band,
    u_out, v_out,
    high, high_left, u_low, u_high, v_low, v_high, sem,
):
    lat = lax.axis_index("lat")
    lon = lax.axis_index("lon")
    groups = levels // group
    width = nlon * lanes
    lane = lax.broadcasted_iota(jnp.int32, (group, lanes), 1)
    middle = pl.ds(group, rows - 2 * group)
    low = pl.ds(0, group)
    top = pl.ds(rows - group, group)
    first = [
        pltpu.make_async_copy(a.at[:, middle], b.at[:, middle], sem.at[k])
        for k, (a, b) in enumerate(((u_part, u_out), (v_part, v_out)))
    ]
    for copy in first:
        copy.start()

    @pl.when(lat == nlat - 1)
    def _():
        start = fold_ref[0]
        own = lax.rem(start - lon * lanes - lane + 2 * width, width)
        before = jnp.zeros_like(lane) + lax.rem(start - lon * lanes + 1 + 2 * width, width)

        def pick(k, part, index):
            block = index // lanes
            spot = index % lanes
            got = jnp.zeros((group, lanes), f32)
            for b in range(nlon):
                taken = jnp.take_along_axis(
                    band[b, k, part, :], spot, axis=1, mode="promise_in_bounds"
                )
                got = jnp.where(block == b, taken, got)
            return -got

        for g in range(groups):
            part = pl.ds(g * group, group)
            for k, source in enumerate((1, 0, 3, 2, 5, 4)):
                high[k, part, :] = pick(source, part, own)
            high_left[part, :] = pick(5, part, before)

    @pl.when(lat < nlat - 1)
    def _():
        for g in range(groups):
            part = pl.ds(g * group, group)
            for k in range(6):
                high[k, part, :] = down_in[k, part, :]
            high_left[part, :] = roll(corner_u[...], lanes - 68 - 4 * g)

    def copy_tiles(l, carry):
        for source, a, b in ((u_part, u_low, u_high), (v_part, v_low, v_high)):
            a[l] = source[l, low, :]
            b[l] = source[l, top, :]
        return carry

    lax.fori_loop(0, levels, copy_tiles, 0, unroll=8)

    views = [ref.reshape(levels * group, lanes) for ref in (u_low, u_high, v_low, v_high)]

    def add(view, g, row, value):
        at = pl.ds(g * group * group + row, group, stride=group)
        view[at, :] = view[at, :] + value

    for g in range(groups):
        part = pl.ds(g * group, group)
        um0, um1, vm0, vm1, _, tv0 = [low_own[k, part, :] for k in range(6)]
        vm30, vm31, tv31 = [high_own[k, part, :] for k in (2, 3, 4)]
        um_2, um_1, vm_2, vm_1, tv_1 = [up_in[k, part, :] for k in range(5)]
        um32, um33, vm32, vm33, tu32, tv32 = [high[k, part, :] for k in range(6)]
        cu0, cu1, cu30, cu31, cv0, cv1, cv30, cv31, tv1, tv30 = [keep[k, part, :] for k in range(10)]
        v0, v30, v31, q_west, q_east = [side[k, part, :] for k in range(5)]

        face = tv_1 + roll(jnp.where(lane == 0, roll(corner_v[...], -(66 + 4 * g)), tv_1), -1)
        f_low = face * q(um_2, um_1, um0, um1)
        d0 = v0 * um_1
        add(views[0], g, 0, -cu0 * (d0 + f_low))
        add(views[0], g, 1, cu1 * d0)
        w_low = (tv_1 + tv0) * q(vm_2, vm_1, vm0, vm1)
        d0 = (tv0 + tv1) * vm_1
        add(views[2], g, 0, -cv0 * (d0 + w_low))
        add(views[2], g, 1, cv1 * d0)
        d30 = v30 * um32
        add(views[1], g, group - 2, -cu30 * d30)
        add(views[1], g, group - 1, cu31 * (v31 * (7.0 * um32 - um33) + d30))
        d30 = (tv30 + tv31) * vm32
        w_high = (tv31 + tv32) * q(vm30, vm31, vm32, vm33)
        tu_west = roll(jnp.where(lane == lanes - 1, high_left[part, :], tu32), 1)
        add(views[3], g, group - 2, -cv30 * d30)
        add(views[3], g, group - 1, cv31 * (w_high + d30 + (tu32 * q_east - tu_west * q_west)))

    last = [
        pltpu.make_async_copy(a, b.at[:, at], sem.at[2 + k])
        for k, (a, b, at) in enumerate((
            (u_low, u_out, low), (u_high, u_out, top), (v_low, v_out, low), (v_high, v_out, top),
        ))
    ]
    for copy in last:
        copy.start()
    for copy in first + last:
        copy.wait()


def local(nlat, nlon, u, v, eu, ev, su, sv, mu, mv, fold):
    u, v, eu, ev, su, sv, mu, mv = [
        pltpu.with_memory_space_constraint(x, pltpu.HBM) for x in (u, v, eu, ev, su, sv, mu, mv)
    ]
    levels, rows, _ = u.shape
    per = lanes // rows
    blocks = levels // per
    chunks = chunk_count(levels, per)
    blocks_in = blocks // chunks
    loads = 3 if chunks % 3 == 0 else chunks
    sides = 1 if nlon == 2 else 2
    pitch = rows + pad
    vmem = pl.BlockSpec(memory_space=pltpu.VMEM)
    hbm = pl.BlockSpec(memory_space=pltpu.HBM)
    block = (levels, rows, lanes)
    line = (levels, lanes)
    shapes = [
        block, block,
        (6,) + line, (6,) + line, (10,) + line, (5,) + line, (5,) + line, (6,) + line,
        (group, lanes), (group, lanes), (nlon, 6) + line,
    ]
    tall = (levels * pitch + pad, lanes)
    turned = (blocks, lanes + 2 * pad, lanes)
    packs = (2, chunks, 6, blocks_in, lanes)
    dma = pltpu.SemaphoreType.DMA
    V = pltpu.VMEM
    fields = pl.pallas_call(
        functools.partial(exchange_kernel, nlat, nlon, levels, rows),
        out_shape=[V(s, f32) for s in shapes],
        in_specs=[hbm] * 8,
        out_specs=[vmem] * len(shapes),
        scratch_shapes=[
            V((4,) + block, f32), V((2,) + block, jnp.int32), V((2, rows, lanes), f32),
            V((4, 4) + line, f32), V((2, 4) + line, jnp.int32),
            V(tall, f32), V(tall, f32), V(block, f32), V(block, f32), V(block, f32),
            V(turned, f32), V(turned, f32), V(turned, f32), V(turned, f32),
            V(packs, f32), V(packs, f32),
            V((group, lanes), f32), V((sides, group, lanes), f32),
            V((chunks, blocks_in, lanes), f32),
            dma((3,)), dma((loads, 2)),
            dma, dma, dma, dma,
            dma((sides,)), dma((chunks, sides)), dma((sides,)), dma((sides,)), dma((2,)), dma((2,)),
            dma((nlon,)), dma((nlon,)),
        ],
        compiler_params=pltpu.CompilerParams(
            collective_id=0, has_side_effects=True, vmem_limit_bytes=36 * 1024 * 1024
        ),
        name="exchange",
    )(u, v, eu, ev, su, sv, mu, mv)
    strip = (levels, group, lanes)
    result = pl.pallas_call(
        functools.partial(finish_kernel, nlat, nlon, levels, rows),
        out_shape=[jax.ShapeDtypeStruct(block, f32)] * 2,
        in_specs=[pl.BlockSpec(memory_space=pltpu.SMEM)] + [vmem] * len(shapes),
        out_specs=[hbm] * 2,
        scratch_shapes=[
            V((6,) + line, f32), V(line, f32),
            V(strip, f32), V(strip, f32), V(strip, f32), V(strip, f32),
            dma((6,)),
        ],
        compiler_params=pltpu.CompilerParams(vmem_limit_bytes=16 * 1024 * 1024),
        name="finish",
    )(fold, *fields)
    return tuple(result)


def solution(mesh):
    level_rows_columns = P(None, "lat", "lon")
    return jax.shard_map(
        functools.partial(local, mesh.shape["lat"], mesh.shape["lon"]),
        mesh=mesh,
        in_specs=(
            level_rows_columns,
            level_rows_columns,
            level_rows_columns,
            level_rows_columns,
            P("lat", "lon"),
            P("lat", "lon"),
            level_rows_columns,
            level_rows_columns,
            P(),
        ),
        out_specs=(level_rows_columns,) * 2,
        check_vma=False,
    )
```

```python
import functools

import jax
import jax.numpy as jnp
from jax import lax
from jax.experimental import pallas as pl
from jax.experimental.pallas import tpu as pltpu
from jax.sharding import PartitionSpec as P

time_step = 0.2
scale = -time_step / 24.0
lanes = 128
group = 8
pad = 8
MESH = pl.DeviceIdType.MESH
f32 = jnp.float32


def chunk_count(levels, per):
    count = levels // per
    return next(c for c in (6, 3, 2, 1) if count % c == 0)


def roll(x, shift):
    return pltpu.roll(x, shift % lanes, 1)


def vroll(x, shift):
    return pltpu.roll(x, shift % group, 0)


def q(a, b, c, d):
    return 7.0 * (b + c) - (a + d)


def exchange_kernel(
    nlat, nlon, levels, rows,
    u_hbm, v_hbm, eu_hbm, ev_hbm, su_hbm, sv_hbm, mu_hbm, mv_hbm,
    u_low, u_mid, u_high, v_low, v_mid, v_high,
    low_own, high_own, keep, side, up_in, down_in, corner_u, corner_v, band,
    real_in, mask_in, span_in,
    edge_f, edge_m, um_n, vm_n, tv_n, cu_n, cv_n, um_t, vm_t, tu_t,
    pack_own, pack_in, edge_own, edge_in, fix,
    early_sem, load_sem, up_send, up_recv, down_send, down_recv,
    lon_send, lon_recv, side_send, side_recv, diag_send, diag_recv, band_send, band_recv,
):
    per = lanes // rows
    tall = rows // group
    blocks = levels // per
    chunks = chunk_count(levels, per)
    blocks_in = blocks // chunks
    groups = levels // group
    pitch = rows + pad
    step = next(n for n in (3, 2, 1) if blocks_in % n == 0)
    loads = 3 if chunks % 3 == 0 else chunks
    depth = levels // loads
    lat = lax.axis_index("lat")
    lon = lax.axis_index("lon")
    right = lax.rem(lon + 1, nlon)
    left = lax.rem(lon + nlon - 1, nlon)
    has_up = lat < nlat - 1
    has_down = lat > 0
    targets = (right,) if nlon == 2 else (right, left)
    sides = len(targets)
    picked = (0, 1, rows - 2, rows - 1)

    reals = (u_hbm, v_hbm, eu_hbm, ev_hbm)
    masks = (mu_hbm, mv_hbm)

    def fetch_edges(sources, edge, sem):
        for k, source in enumerate(sources):
            for e, r in enumerate(picked):
                pltpu.make_async_copy(source.at[:, r, :], edge.at[k, e], sem).start()

    def fetch_part(c):
        part = pl.ds(c * depth, depth)
        for k, source in enumerate(reals):
            pltpu.make_async_copy(source.at[part], real_in.at[k, part], load_sem.at[c, 0]).start(priority=1)
        for k, source in enumerate(masks):
            pltpu.make_async_copy(source.at[part], mask_in.at[k, part], load_sem.at[c, 1]).start(priority=1)

    def landed(ref, sem):
        pltpu.make_async_copy(ref, ref, sem).wait()

    fetch_edges(reals, edge_f, early_sem.at[0])
    fetch_edges(masks, edge_m, early_sem.at[1])
    pltpu.make_async_copy(su_hbm, span_in.at[0], early_sem.at[2]).start()
    pltpu.make_async_copy(sv_hbm, span_in.at[1], early_sem.at[2]).start()
    for c in range(loads):
        fetch_part(c)

    barrier = pltpu.get_barrier_semaphore()

    def greet(where):
        pl.semaphore_signal(barrier, inc=1, device_id=where, device_id_type=MESH)

    greet((lat, right))
    if nlon > 2:
        greet((lat, left))

    @pl.when(has_up)
    def _():
        greet((lat + 1, lon))

    @pl.when(has_down)
    def _():
        greet((lat - 1, lon))

    if nlon > 3:
        @pl.when(lat == nlat - 1)
        def _():
            for d in range(2, nlon - 1):
                greet((lat, lax.rem(lon + d, nlon)))

    def arrive():
        @pl.when(lat == 0)
        def _():
            pl.semaphore_wait(barrier, sides + 1)

        @pl.when(has_up & has_down)
        def _():
            pl.semaphore_wait(barrier, sides + 2)

        @pl.when(lat == nlat - 1)
        def _():
            pl.semaphore_wait(barrier, sides + 1 + max(nlon - 3, 0))

    def remote(src, dst, send, recv, where):
        return pltpu.make_async_remote_copy(
            src_ref=src, dst_ref=dst, send_sem=send, recv_sem=recv,
            device_id=where, device_id_type=MESH,
        )

    def up_copy():
        return remote(high_own.at[pl.ds(0, 5)], up_in, up_send, up_recv, (lat + 1, lon))

    def down_copy():
        return remote(low_own, down_in, down_send, down_recv, (lat - 1, lon))

    cuts = ((pl.ds(0, 11), right),) if nlon == 2 else ((pl.ds(0, 5), right), (pl.ds(5, 6), left))

    def lon_copies(c):
        return [
            remote(pack_own.at[c, cut], pack_in.at[c, cut], lon_send.at[k], lon_recv.at[c, k], (lat, target))
            for k, (cut, target) in enumerate(cuts)
        ]

    def lon_sent():
        return [
            remote(
                pack_own.at[:, cut], pack_in.at[:, cut], lon_send.at[k], lon_recv.at[0, k], (lat, target)
            )
            for k, (cut, target) in enumerate(cuts)
        ]

    def side_copies():
        return [
            remote(edge_own, edge_in.at[k], side_send.at[k], side_recv.at[k], (lat, target))
            for k, target in enumerate(targets)
        ]

    def corner_down():
        return remote(edge_in.at[0], corner_u, diag_send.at[0], diag_recv.at[0], (lat - 1, lon))

    def corner_up():
        return remote(edge_in.at[sides - 1], corner_v, diag_send.at[1], diag_recv.at[1], (lat + 1, lon))

    def band_copy(d, k):
        return remote(
            high_own.at[k], band.at[lon, k], band_send.at[d], band_recv.at[d],
            (lat, lax.rem(lon + d, nlon)),
        )

    def band_sent(d):
        return remote(
            high_own, band.at[lon], band_send.at[d], band_recv.at[d],
            (lat, lax.rem(lon + d, nlon)),
        )

    def band_arrival(d):
        origin = lax.rem(lon + nlon - d, nlon)
        return remote(
            high_own, band.at[origin], band_send.at[d], band_recv.at[d],
            (lat, lax.rem(lon + d, nlon)),
        )

    stages = chunks + 1

    def send_band(stage):
        @pl.when(lat == nlat - 1)
        def _():
            for k in range(4 * stage // stages + 2 * (stage > 0), 4 * (stage + 1) // stages + 2):
                for d in range(1, nlon):
                    band_copy(d, k).start()

    lane = lax.broadcasted_iota(jnp.int32, (group, lanes), 1)
    sub = lax.broadcasted_iota(jnp.int32, (group, lanes), 0)
    zero = jnp.zeros((group, lanes), f32)

    @pl.when(lat == 0)
    def _():
        up_in[...] = jnp.zeros((5, levels, lanes), f32)
        corner_v[...] = zero

    landed(edge_f, early_sem.at[0])
    landed(edge_m, early_sem.at[1])
    landed(span_in, early_sem.at[2])

    def edge_step(g, carry):
        part = pl.ds(pl.multiple_of(g * group, group), group)
        um, vm, tu, tv = [], [], [], []
        for e, r in enumerate(picked):
            mu = edge_m[0, e, part, :].astype(f32)
            mv = edge_m[1, e, part, :].astype(f32)
            um.append(mu * edge_f[0, e, part, :])
            vm.append(mv * edge_f[1, e, part, :])
            vol_u = span_in[0, pl.ds(r, 1), :] * edge_f[2, e, part, :]
            vol_v = span_in[1, pl.ds(r, 1), :] * edge_f[3, e, part, :]
            tu.append(vol_u * um[e])
            tv.append(vol_v * vm[e])
            keep[e, part, :] = mu * scale / vol_u
            keep[4 + e, part, :] = mv * scale / vol_v
        for k, x in enumerate((um[0], um[1], vm[0], vm[1], tu[0], tv[0])):
            low_own[k, part, :] = x
        for k, x in enumerate((um[2], um[3], vm[2], vm[3], tv[3], tu[3])):
            high_own[k, part, :] = x
            band[lon, k, part, :] = x
        keep[8, part, :] = tv[1]
        keep[9, part, :] = tv[2]
        return carry

    lax.fori_loop(0, groups, edge_step, 0)
    ring = zero
    for g in range(groups):
        part = pl.ds(g * group, group)
        tv_top = high_own[4, part, :]
        ring = jnp.where(lane // 4 == g, roll(high_own[3, part, :], 4 * g + 2), ring)
        for k, x in enumerate((low_own[5, part, :], keep[9, part, :], tv_top)):
            ring = jnp.where(lane == 64 + 4 * g + k, roll(x, 64 + 4 * g + k), ring)
        ring = jnp.where(lane == 64 + 4 * g + 3, roll(low_own[4, part, :], 64 + 4 * g + 4), ring)
    edge_own[...] = ring
    def forward():
        for copy in side_copies():
            copy.wait()

        @pl.when(has_down)
        def _():
            corner_down().start()

        @pl.when(has_up)
        def _():
            corner_up().start()

    def begin():
        arrive()

        @pl.when(has_down)
        def _():
            down_copy().start()

        @pl.when(has_up)
        def _():
            up_copy().start()

        send_band(0)

        for copy in side_copies():
            copy.start()

    def clear(l, carry):
        for ref in (um_n, vm_n):
            ref[pl.ds(pl.multiple_of(l * pitch, group), group), :] = zero
        return carry

    lax.fori_loop(0, levels, clear, 0, unroll=8)
    clear(levels, 0)

    begin()

    def prepare(block, c):
        um_b, vm_b, tu_b, tv_b = [], [], [], []
        for s in range(per):
            l = block * per + s
            base = pl.multiple_of(l * pitch + pad, group)
            for b in range(tall):
                at = pl.ds(b * group, group)
                mu = mask_in[0, l, at, :].astype(f32)
                mv = mask_in[1, l, at, :].astype(f32)
                um = mu * real_in[0, l, at, :]
                vm = mv * real_in[1, l, at, :]
                vol_u = span_in[0, at, :] * real_in[2, l, at, :]
                vol_v = span_in[1, at, :] * real_in[3, l, at, :]
                tv = vol_v * vm
                tu_b.append(vol_u * um)
                um_n[pl.ds(base + b * group, group), :] = um
                vm_n[pl.ds(base + b * group, group), :] = vm
                tv_n[l, at, :] = tv
                cu_n[l, at, :] = mu * scale / vol_u
                cv_n[l, at, :] = mv * scale / vol_v
                um_b.append(um)
                vm_b.append(vm)
                tv_b.append(tv)
        here = block - c * blocks_in
        own = pl.ds(here, 1)

        def flip(tiles):
            return jnp.concatenate(tiles, axis=0).T

        for x, ref, first in ((flip(um_b), um_t, 0), (flip(vm_b), vm_t, 2)):
            ref[block, pl.ds(pad, lanes), :] = x
            for k in range(2):
                pack_own[c, first + k, own, :] = x[lanes - 2 + k:lanes - 1 + k]
                pack_own[c, 5 + first + k, own, :] = x[k:k + 1]
        x = flip(tu_b)
        tu_t[block, pl.ds(pad, lanes), :] = x
        pack_own[c, 4, own, :] = x[lanes - 1:]
        pack_own[c, 9, own, :] = x[:1]
        pack_own[c, 10, own, :] = flip(tv_b)[:1]

    def place(parts, b):
        low, middle, high = parts
        if b == 0:
            return low, pl.ds(0, group)
        if b == tall - 1:
            return high, pl.ds(0, group)
        return middle, pl.ds((b - 1) * group, group)

    u_parts = (u_low, u_mid, u_high)
    v_parts = (v_low, v_mid, v_high)

    def inside(block):
        for s in range(per):
            l = block * per + s
            base = l * pitch + pad

            def um(b, shift):
                return um_n[pl.ds(base + b * group + shift, group), :]

            def vm(b, shift):
                return vm_n[pl.ds(base + b * group + shift, group), :]

            f, w, tv_turned = [], [], []
            for b in range(tall):
                at = pl.ds(b * group, group)
                tv = tv_n[l, at, :]
                tv_turned.append(vroll(tv, 1))
                below = jnp.where(sub == 0, tv_turned[b - 1] if b else zero, tv_turned[b])
                f.append((tv + roll(tv, -1)) * q(um(b, -1), um(b, 0), um(b, 1), um(b, 2)))
                cross = (below + tv) * q(vm(b, -2), vm(b, -1), vm(b, 0), vm(b, 1))
                w.append(jnp.where(sub == 0, 0.0, cross) if b == 0 else cross)
            f_turned = [vroll(x, 1) for x in f]
            w_turned = [vroll(x, -1) for x in w] + [zero]
            for b in range(tall):
                at = pl.ds(b * group, group)
                below = jnp.where(sub == 0, f_turned[b - 1] if b else zero, f_turned[b])
                above = jnp.where(sub == group - 1, w_turned[b + 1], w_turned[b])
                ref, to = place(u_parts, b)
                ref[l, to, :] = um(b, 0) + cu_n[l, at, :] * (f[b] - below)
                ref, to = place(v_parts, b)
                ref[l, to, :] = vm(b, 0) + cv_n[l, at, :] * (above - w[b])

    slot = lax.broadcasted_iota(jnp.int32, (blocks_in, lanes), 1) % rows

    def lane_fix(c):
        own = pack_own[c, 1]

        def shifted(x, by):
            keep_it = (slot + by >= 0) & (slot + by < rows)
            return jnp.where(keep_it, pltpu.roll(x, (-by) % lanes, 1), 0.0)

        flux = (pack_in[c, 10] - pack_own[c, 10]) * q(
            shifted(own, -1), own, shifted(own, 1), shifted(own, 2)
        )
        fix[c] = flux - shifted(flux, -1)

    def across(block, c):
        here = pl.ds(block - c * blocks_in, 1)
        for ref, at in ((um_t, 0), (vm_t, 2)):
            for k in range(2):
                ref[block, pl.ds(pad - 2 + k, 1), :] = pack_in[c, at + k, here, :]
                ref[block, pl.ds(pad + lanes + k, 1), :] = pack_in[c, 5 + at + k, here, :]
        tu_t[block, pl.ds(pad - 1, 1), :] = pack_in[c, 4, here, :]
        tu_t[block, pl.ds(pad + lanes, 1), :] = pack_in[c, 9, here, :]

        def read(ref, i):
            return ref[block, pl.ds(pad + i, group), :]

        def west(i):
            return (read(tu_t, i - 1) + read(tu_t, i)) * q(*[read(um_t, i + k) for k in (-2, -1, 0, 1)])

        def east(i):
            tu = read(tu_t, i)
            both = tu + jnp.where(lane % rows == rows - 1, 0.0, roll(tu, -1))
            return both * q(*[read(vm_t, i + k) for k in (-1, 0, 1, 2)])

        count = lanes // group
        fs = [west(i * group) for i in range(count)]
        gs = [east(i * group) for i in range(count)]
        f_turned = [vroll(x, -1) for x in fs] + [west(lanes - group + 1)]
        g_turned = [east(-1)] + [vroll(x, 1) for x in gs]
        du = [
            jnp.where(sub == group - 1, f_turned[i + 1], f_turned[i]) - fs[i] for i in range(count)
        ]
        dv = [gs[i] - jnp.where(sub == 0, g_turned[i], g_turned[i + 1]) for i in range(count)]
        du[-1] = du[-1] + jnp.where(sub == group - 1, fix[c, here, :], 0.0)
        du = jnp.concatenate(du, axis=0).T
        dv = jnp.concatenate(dv, axis=0).T
        for s in range(per):
            l = block * per + s
            for b in range(tall):
                at = pl.ds(b * group, group)
                k = (s * tall + b) * group
                for parts, c_n, d in ((u_parts, cu_n, du), (v_parts, cv_n, dv)):
                    ref, to = place(parts, b)
                    ref[l, to, :] = ref[l, to, :] + c_n[l, at, :] * d[k:k + group]

    def every(body, c):
        def run(i, carry):
            for k in range(step):
                body(i * step + k)
            return carry

        lax.fori_loop(c * blocks_in // step, (c + 1) * blocks_in // step, run, 0)

    for c in range(chunks):
        if c * loads % chunks == 0:
            part = pl.ds(c * loads // chunks * depth, depth)
            landed(real_in.at[:, part], load_sem.at[c * loads // chunks, 0])
            landed(mask_in.at[:, part], load_sem.at[c * loads // chunks, 1])
        every(lambda i: prepare(i, c), c)
        for copy in lon_copies(c):
            copy.start()
        send_band(c + 1)
    for c in range(chunks):
        every(inside, c)
        if c == (chunks - 1) // 2:
            forward()

    for g in range(groups):
        part = pl.ds(g * group, group)
        from_left, from_right = edge_in[0], edge_in[sides - 1]
        for k, x in enumerate((low_own[5, part, :], keep[9, part, :], high_own[4, part, :])):
            halo = roll(from_right, -(64 + 4 * g + k))
            side[k, part, :] = x + roll(jnp.where(lane == 0, halo, x), -1)
        vm = high_own[3, part, :]
        halo = roll(jnp.where(lane % 4 < 2, from_left, from_right), -(4 * g + 2))
        w2 = roll(jnp.where(lane >= lanes - 2, halo, vm), 2)
        w1 = roll(jnp.where(lane == lanes - 1, halo, vm), 1)
        e1 = roll(jnp.where(lane == 0, halo, vm), -1)
        e2 = roll(jnp.where(lane < 2, halo, vm), -2)
        side[3, part, :] = q(w2, w1, vm, e1)
        side[4, part, :] = q(w1, vm, e1, e2)

    for c in range(chunks):
        for copy in lon_copies(c):
            copy.wait_recv()
        lane_fix(c)
        every(lambda i: across(i, c), c)

    for copy in lon_sent():
        copy.wait_send()

    @pl.when(has_down)
    def _():
        down_copy().wait_send()
        corner_down().wait_send()
        up_copy().wait_recv()
        corner_up().wait_recv()

    @pl.when(has_up)
    def _():
        up_copy().wait_send()
        corner_up().wait_send()
        down_copy().wait_recv()
        corner_down().wait_recv()

    @pl.when(lat == nlat - 1)
    def _():
        for d in range(1, nlon):
            band_sent(d).wait_send()
            band_arrival(d).wait_recv()


def finish_kernel(
    nlat, nlon, levels, rows,
    fold_ref, u_mid, v_mid, low_own, high_own, keep, side, up_in, corner_u, corner_v, band,
    u_low_in, u_high_in, v_low_in, v_high_in, down_in,
    u_out, v_out, u_low, u_high, v_low, v_high, high,
    high_left, sem,
):
    lat = lax.axis_index("lat")
    lon = lax.axis_index("lon")
    groups = levels // group
    width = nlon * lanes
    lane = lax.broadcasted_iota(jnp.int32, (group, lanes), 1)
    top = lat == nlat - 1
    low_rows = pl.ds(0, group)
    high_rows = pl.ds(rows - group, group)
    middle = pl.ds(group, rows - 2 * group)
    copies = [
        pltpu.make_async_copy(a, b.at[:, at], sem.at[k])
        for k, (a, b, at) in enumerate((
            (u_mid, u_out, middle), (v_mid, v_out, middle),
            (u_low, u_out, low_rows), (u_high, u_out, high_rows),
            (v_low, v_out, low_rows), (v_high, v_out, high_rows),
        ))
    ]
    for copy in copies[:2]:
        copy.start()

    @pl.when(top)
    def _():
        start = fold_ref[0]
        own = lax.rem(start - lon * lanes - lane + 2 * width, width)
        before = jnp.zeros_like(lane) + lax.rem(start - lon * lanes + 1 + 2 * width, width)

        def pick(k, part, index):
            block = index // lanes
            spot = index % lanes
            got = jnp.zeros((group, lanes), f32)
            for b in range(nlon):
                taken = jnp.take_along_axis(
                    band[b, k, part, :], spot, axis=1, mode="promise_in_bounds"
                )
                got = jnp.where(block == b, taken, got)
            return -got

        for g in range(groups):
            part = pl.ds(g * group, group)
            for k, source in enumerate((1, 0, 3, 2, 5, 4)):
                high[k, part, :] = pick(source, part, own)
            high_left[part, :] = pick(5, part, before)

    def add(ref, g, row, value):
        view = ref.reshape(levels * group, lanes)
        at = pl.ds(g * group * group + row, group, stride=group)
        view[at, :] = view[at, :] + value

    for g in range(groups):
        part = pl.ds(g * group, group)
        um0, um1 = low_own[0, part, :], low_own[1, part, :]
        um_2, um_1, tv_1 = [up_in[k, part, :] for k in (0, 1, 4)]
        um32, um33 = high[0, part, :], high[1, part, :]
        cu0, cu1, cu30, cu31 = [keep[k, part, :] for k in range(4)]
        v0, v30, v31 = [side[k, part, :] for k in range(3)]
        corner = roll(corner_v[...], -(66 + 4 * g))
        face = tv_1 + roll(jnp.where(lane == 0, corner, tv_1), -1)
        f_low = face * q(um_2, um_1, um0, um1)
        d0 = v0 * um_1
        add(u_low, g, 0, -cu0 * (d0 + f_low))
        add(u_low, g, 1, cu1 * d0)
        d30 = v30 * um32
        add(u_high, g, group - 2, -cu30 * d30)
        add(u_high, g, group - 1, cu31 * (v31 * (7.0 * um32 - um33) + d30))
    for copy in copies[2:4]:
        copy.start()

    for g in range(groups):
        part = pl.ds(g * group, group)
        vm0, vm1, tv0 = [low_own[k, part, :] for k in (2, 3, 5)]
        vm30, vm31, tv31 = [high_own[k, part, :] for k in (2, 3, 4)]
        vm_2, vm_1, tv_1 = [up_in[k, part, :] for k in (2, 3, 4)]
        vm32, vm33, tu32, tv32 = [high[k, part, :] for k in (2, 3, 4, 5)]
        cv0, cv1, cv30, cv31, tv1, tv30 = [keep[k, part, :] for k in range(4, 10)]
        q_west, q_east = side[3, part, :], side[4, part, :]
        w_low = (tv_1 + tv0) * q(vm_2, vm_1, vm0, vm1)
        d0 = (tv0 + tv1) * vm_1
        add(v_low, g, 0, -cv0 * (d0 + w_low))
        add(v_low, g, 1, cv1 * d0)
        d30 = (tv30 + tv31) * vm32
        w_high = (tv31 + tv32) * q(vm30, vm31, vm32, vm33)
        corner = jnp.where(top, high_left[part, :], roll(corner_u[...], lanes - 68 - 4 * g))
        tu_west = roll(jnp.where(lane == lanes - 1, corner, tu32), 1)
        add(v_high, g, group - 2, -cv30 * d30)
        add(v_high, g, group - 1, cv31 * (w_high + d30 + (tu32 * q_east - tu_west * q_west)))
    for copy in copies[4:]:
        copy.start()
    for copy in copies:
        copy.wait()


def local(nlat, nlon, u, v, eu, ev, su, sv, mu, mv, fold):
    u, v, eu, ev, su, sv, mu, mv = [
        pltpu.with_memory_space_constraint(x, pltpu.HBM) for x in (u, v, eu, ev, su, sv, mu, mv)
    ]
    levels, rows, _ = u.shape
    per = lanes // rows
    blocks = levels // per
    chunks = chunk_count(levels, per)
    blocks_in = blocks // chunks
    loads = 3 if chunks % 3 == 0 else chunks
    sides = 1 if nlon == 2 else 2
    pitch = rows + pad
    vmem = pl.BlockSpec(memory_space=pltpu.VMEM)
    hbm = pl.BlockSpec(memory_space=pltpu.HBM)
    block = (levels, rows, lanes)
    line = (levels, lanes)
    strip = (levels, group, lanes)
    shapes = [
        strip, (levels, rows - 2 * group, lanes), strip,
        strip, (levels, rows - 2 * group, lanes), strip,
        (6,) + line, (6,) + line, (10,) + line, (5,) + line, (5,) + line, (6,) + line,
        (group, lanes), (group, lanes), (nlon, 6) + line,
    ]
    tall = (levels * pitch + pad, lanes)
    turned = (blocks, lanes + 2 * pad, lanes)
    packs = (chunks, 11, blocks_in, lanes)
    dma = pltpu.SemaphoreType.DMA
    V = pltpu.VMEM
    fields = pl.pallas_call(
        functools.partial(exchange_kernel, nlat, nlon, levels, rows),
        out_shape=[V(s, f32) for s in shapes],
        in_specs=[hbm] * 8,
        out_specs=[vmem] * len(shapes),
        scratch_shapes=[
            V((4,) + block, f32), V((2,) + block, jnp.int32), V((2, rows, lanes), f32),
            V((4, 4) + line, f32), V((2, 4) + line, jnp.int32),
            V(tall, f32), V(tall, f32), V(block, f32), V(block, f32), V(block, f32),
            V(turned, f32), V(turned, f32), V(turned, f32),
            V(packs, f32), V(packs, f32),
            V((group, lanes), f32), V((sides, group, lanes), f32),
            V((chunks, blocks_in, lanes), f32),
            dma((3,)), dma((loads, 2)),
            dma, dma, dma, dma,
            dma((sides,)), dma((chunks, sides)), dma((sides,)), dma((sides,)), dma((2,)), dma((2,)),
            dma((nlon,)), dma((nlon,)),
        ],
        compiler_params=pltpu.CompilerParams(
            collective_id=0, has_side_effects=True, vmem_limit_bytes=36 * 1024 * 1024
        ),
        name="exchange",
    )(u, v, eu, ev, su, sv, mu, mv)
    u_low, u_mid, u_high, v_low, v_mid, v_high = fields[:6]
    low_own, high_own, keep, side, up_in, down_in, corner_u, corner_v, band = fields[6:]
    changed = (u_low, u_high, v_low, v_high, down_in)
    fixed = (u_mid, v_mid, low_own, high_own, keep, side, up_in, corner_u, corner_v, band)
    result = pl.pallas_call(
        functools.partial(finish_kernel, nlat, nlon, levels, rows),
        out_shape=[jax.ShapeDtypeStruct(block, f32)] * 2 + [V(x.shape, f32) for x in changed],
        in_specs=[pl.BlockSpec(memory_space=pltpu.SMEM)] + [vmem] * (len(fixed) + len(changed)),
        out_specs=[hbm] * 2 + [vmem] * len(changed),
        input_output_aliases={1 + len(fixed) + k: 2 + k for k in range(len(changed))},
        scratch_shapes=[V(line, f32), dma((6,))],
        compiler_params=pltpu.CompilerParams(vmem_limit_bytes=16 * 1024 * 1024),
        name="finish",
    )(fold, *fixed, *changed)
    return tuple(result[:2])


def solution(mesh):
    level_rows_columns = P(None, "lat", "lon")
    return jax.shard_map(
        functools.partial(local, mesh.shape["lat"], mesh.shape["lon"]),
        mesh=mesh,
        in_specs=(
            level_rows_columns,
            level_rows_columns,
            level_rows_columns,
            level_rows_columns,
            P("lat", "lon"),
            P("lat", "lon"),
            level_rows_columns,
            level_rows_columns,
            P(),
        ),
        out_specs=(level_rows_columns,) * 2,
        check_vma=False,
    )
```

```python
import functools

import jax
import jax.numpy as jnp
from jax import lax
from jax.experimental import pallas as pl
from jax.experimental.pallas import tpu as pltpu
from jax.sharding import PartitionSpec as P

time_step = 0.2
scale = -time_step / 24.0
lanes = 128
group = 8
pad = 8
MESH = pl.DeviceIdType.MESH
f32 = jnp.float32


def chunk_count(levels, per):
    count = levels // per
    return next(c for c in (6, 3, 2, 1) if count % c == 0)


def roll(x, shift):
    return pltpu.roll(x, shift % lanes, 1)


def vroll(x, shift):
    return pltpu.roll(x, shift % group, 0)


def q(a, b, c, d):
    return 7.0 * (b + c) - (a + d)


def exchange_kernel(
    nlat, nlon, levels, rows,
    u_hbm, v_hbm, eu_hbm, ev_hbm, su_hbm, sv_hbm, mu_hbm, mv_hbm,
    u_low, u_mid, u_high, v_low, v_mid, v_high,
    low_own, high_own, keep, side, up_in, down_in, corner_u, corner_v, band,
    real_in, mask_in, span_in,
    edge_f, edge_m, um_n, vm_n, tv_n, cu_n, cv_n, um_t, vm_t, tu_t,
    pack_own, pack_in, edge_own, edge_in, fix,
    early_sem, load_sem, up_send, up_recv, down_send, down_recv,
    lon_send, lon_recv, side_send, side_recv, diag_send, diag_recv, band_send, band_recv,
):
    per = lanes // rows
    tall = rows // group
    blocks = levels // per
    chunks = chunk_count(levels, per)
    blocks_in = blocks // chunks
    groups = levels // group
    pitch = rows + pad
    step = next(n for n in (3, 2, 1) if blocks_in % n == 0)
    loads = chunks
    depth = levels // loads
    lat = lax.axis_index("lat")
    lon = lax.axis_index("lon")
    right = lax.rem(lon + 1, nlon)
    left = lax.rem(lon + nlon - 1, nlon)
    has_up = lat < nlat - 1
    has_down = lat > 0
    targets = (right,) if nlon == 2 else (right, left)
    sides = len(targets)
    picked = (0, 1, rows - 2, rows - 1)

    reals = (u_hbm, v_hbm, eu_hbm, ev_hbm)
    masks = (mu_hbm, mv_hbm)

    def fetch_edges(sources, edge, sem):
        for k, source in enumerate(sources):
            for e, r in enumerate(picked):
                pltpu.make_async_copy(source.at[:, r, :], edge.at[k, e], sem).start()

    def fetch_part(c):
        part = pl.ds(c * depth, depth)
        for k, source in enumerate(reals):
            pltpu.make_async_copy(source.at[part], real_in.at[k, part], load_sem.at[c, 0]).start(priority=1)
        for k, source in enumerate(masks):
            pltpu.make_async_copy(source.at[part], mask_in.at[k, part], load_sem.at[c, 1]).start(priority=1)

    def landed(ref, sem):
        pltpu.make_async_copy(ref, ref, sem).wait()

    fetch_edges(reals, edge_f, early_sem.at[0])
    fetch_edges(masks, edge_m, early_sem.at[1])
    pltpu.make_async_copy(su_hbm, span_in.at[0], early_sem.at[2]).start()
    pltpu.make_async_copy(sv_hbm, span_in.at[1], early_sem.at[2]).start()
    for c in range(loads):
        fetch_part(c)

    barrier = pltpu.get_barrier_semaphore()

    def greet(where):
        pl.semaphore_signal(barrier, inc=1, device_id=where, device_id_type=MESH)

    greet((lat, right))
    if nlon > 2:
        greet((lat, left))

    @pl.when(has_up)
    def _():
        greet((lat + 1, lon))

    @pl.when(has_down)
    def _():
        greet((lat - 1, lon))

    if nlon > 3:
        @pl.when(lat == nlat - 1)
        def _():
            for d in range(2, nlon - 1):
                greet((lat, lax.rem(lon + d, nlon)))

    def arrive():
        @pl.when(lat == 0)
        def _():
            pl.semaphore_wait(barrier, sides + 1)

        @pl.when(has_up & has_down)
        def _():
            pl.semaphore_wait(barrier, sides + 2)

        @pl.when(lat == nlat - 1)
        def _():
            pl.semaphore_wait(barrier, sides + 1 + max(nlon - 3, 0))

    def remote(src, dst, send, recv, where):
        return pltpu.make_async_remote_copy(
            src_ref=src, dst_ref=dst, send_sem=send, recv_sem=recv,
            device_id=where, device_id_type=MESH,
        )

    def up_copy():
        return remote(high_own.at[pl.ds(0, 5)], up_in, up_send, up_recv, (lat + 1, lon))

    def down_copy():
        return remote(low_own, down_in, down_send, down_recv, (lat - 1, lon))

    cuts = ((pl.ds(0, 11), right),) if nlon == 2 else ((pl.ds(0, 5), right), (pl.ds(5, 6), left))

    def lon_copies(c):
        return [
            remote(pack_own.at[c, cut], pack_in.at[c, cut], lon_send.at[k], lon_recv.at[c, k], (lat, target))
            for k, (cut, target) in enumerate(cuts)
        ]

    def lon_sent():
        return [
            remote(
                pack_own.at[:, cut], pack_in.at[:, cut], lon_send.at[k], lon_recv.at[0, k], (lat, target)
            )
            for k, (cut, target) in enumerate(cuts)
        ]

    def side_copies():
        return [
            remote(edge_own, edge_in.at[k], side_send.at[k], side_recv.at[k], (lat, target))
            for k, target in enumerate(targets)
        ]

    def corner_down():
        return remote(edge_in.at[0], corner_u, diag_send.at[0], diag_recv.at[0], (lat - 1, lon))

    def corner_up():
        return remote(edge_in.at[sides - 1], corner_v, diag_send.at[1], diag_recv.at[1], (lat + 1, lon))

    def band_copy(d, k):
        return remote(
            high_own.at[k], band.at[lon, k], band_send.at[d], band_recv.at[d],
            (lat, lax.rem(lon + d, nlon)),
        )

    def band_sent(d):
        return remote(
            high_own, band.at[lon], band_send.at[d], band_recv.at[d],
            (lat, lax.rem(lon + d, nlon)),
        )

    def band_arrival(d):
        origin = lax.rem(lon + nlon - d, nlon)
        return remote(
            high_own, band.at[origin], band_send.at[d], band_recv.at[d],
            (lat, lax.rem(lon + d, nlon)),
        )

    stages = chunks + 1

    def send_band(stage):
        @pl.when(lat == nlat - 1)
        def _():
            for k in range(4 * stage // stages + 2 * (stage > 0), 4 * (stage + 1) // stages + 2):
                for d in range(1, nlon):
                    band_copy(d, k).start()

    lane = lax.broadcasted_iota(jnp.int32, (group, lanes), 1)
    sub = lax.broadcasted_iota(jnp.int32, (group, lanes), 0)
    zero = jnp.zeros((group, lanes), f32)

    @pl.when(lat == 0)
    def _():
        up_in[...] = jnp.zeros((5, levels, lanes), f32)
        corner_v[...] = zero

    landed(edge_f, early_sem.at[0])
    landed(edge_m, early_sem.at[1])
    landed(span_in, early_sem.at[2])

    def edge_step(g, carry):
        part = pl.ds(pl.multiple_of(g * group, group), group)
        um, vm, tu, tv = [], [], [], []
        for e, r in enumerate(picked):
            mu = edge_m[0, e, part, :].astype(f32)
            mv = edge_m[1, e, part, :].astype(f32)
            um.append(mu * edge_f[0, e, part, :])
            vm.append(mv * edge_f[1, e, part, :])
            vol_u = span_in[0, pl.ds(r, 1), :] * edge_f[2, e, part, :]
            vol_v = span_in[1, pl.ds(r, 1), :] * edge_f[3, e, part, :]
            tu.append(vol_u * um[e])
            tv.append(vol_v * vm[e])
            keep[e, part, :] = mu * scale / vol_u
            keep[4 + e, part, :] = mv * scale / vol_v
        for k, x in enumerate((um[0], um[1], vm[0], vm[1], tu[0], tv[0])):
            low_own[k, part, :] = x
        for k, x in enumerate((um[2], um[3], vm[2], vm[3], tv[3], tu[3])):
            high_own[k, part, :] = x
            band[lon, k, part, :] = x
        keep[8, part, :] = tv[1]
        keep[9, part, :] = tv[2]
        return carry

    lax.fori_loop(0, groups, edge_step, 0)
    ring = zero
    for g in range(groups):
        part = pl.ds(g * group, group)
        tv_top = high_own[4, part, :]
        ring = jnp.where(lane // 4 == g, roll(high_own[3, part, :], 4 * g + 2), ring)
        for k, x in enumerate((low_own[5, part, :], keep[9, part, :], tv_top)):
            ring = jnp.where(lane == 64 + 4 * g + k, roll(x, 64 + 4 * g + k), ring)
        ring = jnp.where(lane == 64 + 4 * g + 3, roll(low_own[4, part, :], 64 + 4 * g + 4), ring)
    edge_own[...] = ring
    def forward():
        for copy in side_copies():
            copy.wait()

        @pl.when(has_down)
        def _():
            corner_down().start()

        @pl.when(has_up)
        def _():
            corner_up().start()

    def begin():
        arrive()

        @pl.when(has_down)
        def _():
            down_copy().start()

        @pl.when(has_up)
        def _():
            up_copy().start()

        send_band(0)

        for copy in side_copies():
            copy.start()

    def clear(l, carry):
        for ref in (um_n, vm_n):
            ref[pl.ds(pl.multiple_of(l * pitch, group), group), :] = zero
        return carry

    lax.fori_loop(0, levels, clear, 0, unroll=8)
    clear(levels, 0)

    begin()

    def prepare(block, c):
        um_b, vm_b, tu_b, tv_b = [], [], [], []
        for s in range(per):
            l = block * per + s
            base = pl.multiple_of(l * pitch + pad, group)
            for b in range(tall):
                at = pl.ds(b * group, group)
                mu = mask_in[0, l, at, :].astype(f32)
                mv = mask_in[1, l, at, :].astype(f32)
                um = mu * real_in[0, l, at, :]
                vm = mv * real_in[1, l, at, :]
                vol_u = span_in[0, at, :] * real_in[2, l, at, :]
                vol_v = span_in[1, at, :] * real_in[3, l, at, :]
                tv = vol_v * vm
                tu_b.append(vol_u * um)
                um_n[pl.ds(base + b * group, group), :] = um
                vm_n[pl.ds(base + b * group, group), :] = vm
                tv_n[l, at, :] = tv
                cu_n[l, at, :] = mu * scale / vol_u
                cv_n[l, at, :] = mv * scale / vol_v
                um_b.append(um)
                vm_b.append(vm)
                tv_b.append(tv)
        here = block - c * blocks_in
        own = pl.ds(here, 1)

        def flip(tiles):
            return jnp.concatenate(tiles, axis=0).T

        for x, ref, first in ((flip(um_b), um_t, 0), (flip(vm_b), vm_t, 2)):
            ref[block, pl.ds(pad, lanes), :] = x
            for k in range(2):
                pack_own[c, first + k, own, :] = x[lanes - 2 + k:lanes - 1 + k]
                pack_own[c, 5 + first + k, own, :] = x[k:k + 1]
        x = flip(tu_b)
        tu_t[block, pl.ds(pad, lanes), :] = x
        pack_own[c, 4, own, :] = x[lanes - 1:]
        pack_own[c, 9, own, :] = x[:1]
        pack_own[c, 10, own, :] = flip(tv_b)[:1]

    def place(parts, b):
        low, middle, high = parts
        if b == 0:
            return low, pl.ds(0, group)
        if b == tall - 1:
            return high, pl.ds(0, group)
        return middle, pl.ds((b - 1) * group, group)

    u_parts = (u_low, u_mid, u_high)
    v_parts = (v_low, v_mid, v_high)

    def inside(block):
        for s in range(per):
            l = block * per + s
            base = l * pitch + pad

            def um(b, shift):
                return um_n[pl.ds(base + b * group + shift, group), :]

            def vm(b, shift):
                return vm_n[pl.ds(base + b * group + shift, group), :]

            f, w, tv_turned = [], [], []
            for b in range(tall):
                at = pl.ds(b * group, group)
                tv = tv_n[l, at, :]
                tv_turned.append(vroll(tv, 1))
                below = jnp.where(sub == 0, tv_turned[b - 1] if b else zero, tv_turned[b])
                f.append((tv + roll(tv, -1)) * q(um(b, -1), um(b, 0), um(b, 1), um(b, 2)))
                cross = (below + tv) * q(vm(b, -2), vm(b, -1), vm(b, 0), vm(b, 1))
                w.append(jnp.where(sub == 0, 0.0, cross) if b == 0 else cross)
            f_turned = [vroll(x, 1) for x in f]
            w_turned = [vroll(x, -1) for x in w] + [zero]
            for b in range(tall):
                at = pl.ds(b * group, group)
                below = jnp.where(sub == 0, f_turned[b - 1] if b else zero, f_turned[b])
                above = jnp.where(sub == group - 1, w_turned[b + 1], w_turned[b])
                ref, to = place(u_parts, b)
                ref[l, to, :] = um(b, 0) + cu_n[l, at, :] * (f[b] - below)
                ref, to = place(v_parts, b)
                ref[l, to, :] = vm(b, 0) + cv_n[l, at, :] * (above - w[b])

    slot = lax.broadcasted_iota(jnp.int32, (blocks_in, lanes), 1) % rows

    def lane_fix(c):
        own = pack_own[c, 1]

        def shifted(x, by):
            keep_it = (slot + by >= 0) & (slot + by < rows)
            return jnp.where(keep_it, pltpu.roll(x, (-by) % lanes, 1), 0.0)

        flux = (pack_in[c, 10] - pack_own[c, 10]) * q(
            shifted(own, -1), own, shifted(own, 1), shifted(own, 2)
        )
        fix[c] = flux - shifted(flux, -1)

    def across(block, c):
        here = pl.ds(block - c * blocks_in, 1)
        for ref, at in ((um_t, 0), (vm_t, 2)):
            for k in range(2):
                ref[block, pl.ds(pad - 2 + k, 1), :] = pack_in[c, at + k, here, :]
                ref[block, pl.ds(pad + lanes + k, 1), :] = pack_in[c, 5 + at + k, here, :]
        tu_t[block, pl.ds(pad - 1, 1), :] = pack_in[c, 4, here, :]
        tu_t[block, pl.ds(pad + lanes, 1), :] = pack_in[c, 9, here, :]

        def read(ref, i):
            return ref[block, pl.ds(pad + i, group), :]

        def west(i):
            return (read(tu_t, i - 1) + read(tu_t, i)) * q(*[read(um_t, i + k) for k in (-2, -1, 0, 1)])

        def east(i):
            tu = read(tu_t, i)
            both = tu + jnp.where(lane % rows == rows - 1, 0.0, roll(tu, -1))
            return both * q(*[read(vm_t, i + k) for k in (-1, 0, 1, 2)])

        count = lanes // group
        fs = [west(i * group) for i in range(count)]
        gs = [east(i * group) for i in range(count)]
        f_turned = [vroll(x, -1) for x in fs] + [west(lanes - group + 1)]
        g_turned = [east(-1)] + [vroll(x, 1) for x in gs]
        du = [
            jnp.where(sub == group - 1, f_turned[i + 1], f_turned[i]) - fs[i] for i in range(count)
        ]
        dv = [gs[i] - jnp.where(sub == 0, g_turned[i], g_turned[i + 1]) for i in range(count)]
        du[-1] = du[-1] + jnp.where(sub == group - 1, fix[c, here, :], 0.0)
        du = jnp.concatenate(du, axis=0).T
        dv = jnp.concatenate(dv, axis=0).T
        for s in range(per):
            l = block * per + s
            for b in range(tall):
                at = pl.ds(b * group, group)
                k = (s * tall + b) * group
                for parts, c_n, d in ((u_parts, cu_n, du), (v_parts, cv_n, dv)):
                    ref, to = place(parts, b)
                    ref[l, to, :] = ref[l, to, :] + c_n[l, at, :] * d[k:k + group]

    def every(body, c):
        def run(i, carry):
            for k in range(step):
                body(i * step + k)
            return carry

        lax.fori_loop(c * blocks_in // step, (c + 1) * blocks_in // step, run, 0)

    for c in range(chunks):
        if c * loads % chunks == 0:
            part = pl.ds(c * loads // chunks * depth, depth)
            landed(real_in.at[:, part], load_sem.at[c * loads // chunks, 0])
            landed(mask_in.at[:, part], load_sem.at[c * loads // chunks, 1])
        every(lambda i: prepare(i, c), c)
        for copy in lon_copies(c):
            copy.start()
        send_band(c + 1)
    for c in range(chunks):
        every(inside, c)
    forward()

    for g in range(groups):
        part = pl.ds(g * group, group)
        from_left, from_right = edge_in[0], edge_in[sides - 1]
        for k, x in enumerate((low_own[5, part, :], keep[9, part, :], high_own[4, part, :])):
            halo = roll(from_right, -(64 + 4 * g + k))
            side[k, part, :] = x + roll(jnp.where(lane == 0, halo, x), -1)
        vm = high_own[3, part, :]
        halo = roll(jnp.where(lane % 4 < 2, from_left, from_right), -(4 * g + 2))
        w2 = roll(jnp.where(lane >= lanes - 2, halo, vm), 2)
        w1 = roll(jnp.where(lane == lanes - 1, halo, vm), 1)
        e1 = roll(jnp.where(lane == 0, halo, vm), -1)
        e2 = roll(jnp.where(lane < 2, halo, vm), -2)
        side[3, part, :] = q(w2, w1, vm, e1)
        side[4, part, :] = q(w1, vm, e1, e2)

    for c in range(chunks):
        for copy in lon_copies(c):
            copy.wait_recv()
        lane_fix(c)
        every(lambda i: across(i, c), c)

    for copy in lon_sent():
        copy.wait_send()

    @pl.when(has_down)
    def _():
        down_copy().wait_send()
        corner_down().wait_send()
        up_copy().wait_recv()
        corner_up().wait_recv()

    @pl.when(has_up)
    def _():
        up_copy().wait_send()
        corner_up().wait_send()
        down_copy().wait_recv()
        corner_down().wait_recv()

    @pl.when(lat == nlat - 1)
    def _():
        for d in range(1, nlon):
            band_sent(d).wait_send()
            band_arrival(d).wait_recv()


def finish_kernel(
    nlat, nlon, levels, rows,
    fold_ref, u_mid, v_mid, low_own, high_own, keep, side, up_in, corner_u, corner_v, band,
    u_low_in, u_high_in, v_low_in, v_high_in, down_in,
    u_out, v_out, u_low, u_high, v_low, v_high, high,
    high_left, sem,
):
    lat = lax.axis_index("lat")
    lon = lax.axis_index("lon")
    groups = levels // group
    width = nlon * lanes
    lane = lax.broadcasted_iota(jnp.int32, (group, lanes), 1)
    top = lat == nlat - 1
    low_rows = pl.ds(0, group)
    high_rows = pl.ds(rows - group, group)
    middle = pl.ds(group, rows - 2 * group)
    copies = [
        pltpu.make_async_copy(a, b.at[:, at], sem.at[k])
        for k, (a, b, at) in enumerate((
            (u_mid, u_out, middle), (v_mid, v_out, middle),
            (u_low, u_out, low_rows), (u_high, u_out, high_rows),
            (v_low, v_out, low_rows), (v_high, v_out, high_rows),
        ))
    ]
    for copy in copies[:2]:
        copy.start()

    @pl.when(top)
    def _():
        start = fold_ref[0]
        own = lax.rem(start - lon * lanes - lane + 2 * width, width)
        before = jnp.zeros_like(lane) + lax.rem(start - lon * lanes + 1 + 2 * width, width)

        def pick(k, part, index):
            block = index // lanes
            spot = index % lanes
            got = jnp.zeros((group, lanes), f32)
            for b in range(nlon):
                taken = jnp.take_along_axis(
                    band[b, k, part, :], spot, axis=1, mode="promise_in_bounds"
                )
                got = jnp.where(block == b, taken, got)
            return -got

        for g in range(groups):
            part = pl.ds(g * group, group)
            for k, source in enumerate((1, 0, 3, 2, 5, 4)):
                high[k, part, :] = pick(source, part, own)
            high_left[part, :] = pick(5, part, before)

    def add(ref, g, row, value):
        view = ref.reshape(levels * group, lanes)
        at = pl.ds(g * group * group + row, group, stride=group)
        view[at, :] = view[at, :] + value

    for g in range(groups):
        part = pl.ds(g * group, group)
        um0, um1 = low_own[0, part, :], low_own[1, part, :]
        um_2, um_1, tv_1 = [up_in[k, part, :] for k in (0, 1, 4)]
        um32, um33 = high[0, part, :], high[1, part, :]
        cu0, cu1, cu30, cu31 = [keep[k, part, :] for k in range(4)]
        v0, v30, v31 = [side[k, part, :] for k in range(3)]
        corner = roll(corner_v[...], -(66 + 4 * g))
        face = tv_1 + roll(jnp.where(lane == 0, corner, tv_1), -1)
        f_low = face * q(um_2, um_1, um0, um1)
        d0 = v0 * um_1
        add(u_low, g, 0, -cu0 * (d0 + f_low))
        add(u_low, g, 1, cu1 * d0)
        d30 = v30 * um32
        add(u_high, g, group - 2, -cu30 * d30)
        add(u_high, g, group - 1, cu31 * (v31 * (7.0 * um32 - um33) + d30))
    for copy in copies[2:4]:
        copy.start()

    for g in range(groups):
        part = pl.ds(g * group, group)
        vm0, vm1, tv0 = [low_own[k, part, :] for k in (2, 3, 5)]
        vm30, vm31, tv31 = [high_own[k, part, :] for k in (2, 3, 4)]
        vm_2, vm_1, tv_1 = [up_in[k, part, :] for k in (2, 3, 4)]
        vm32, vm33, tu32, tv32 = [high[k, part, :] for k in (2, 3, 4, 5)]
        cv0, cv1, cv30, cv31, tv1, tv30 = [keep[k, part, :] for k in range(4, 10)]
        q_west, q_east = side[3, part, :], side[4, part, :]
        w_low = (tv_1 + tv0) * q(vm_2, vm_1, vm0, vm1)
        d0 = (tv0 + tv1) * vm_1
        add(v_low, g, 0, -cv0 * (d0 + w_low))
        add(v_low, g, 1, cv1 * d0)
        d30 = (tv30 + tv31) * vm32
        w_high = (tv31 + tv32) * q(vm30, vm31, vm32, vm33)
        corner = jnp.where(top, high_left[part, :], roll(corner_u[...], lanes - 68 - 4 * g))
        tu_west = roll(jnp.where(lane == lanes - 1, corner, tu32), 1)
        add(v_high, g, group - 2, -cv30 * d30)
        add(v_high, g, group - 1, cv31 * (w_high + d30 + (tu32 * q_east - tu_west * q_west)))
    for copy in copies[4:]:
        copy.start()
    for copy in copies:
        copy.wait()


def local(nlat, nlon, u, v, eu, ev, su, sv, mu, mv, fold):
    u, v, eu, ev, su, sv, mu, mv = [
        pltpu.with_memory_space_constraint(x, pltpu.HBM) for x in (u, v, eu, ev, su, sv, mu, mv)
    ]
    levels, rows, _ = u.shape
    per = lanes // rows
    blocks = levels // per
    chunks = chunk_count(levels, per)
    blocks_in = blocks // chunks
    loads = chunks
    sides = 1 if nlon == 2 else 2
    pitch = rows + pad
    vmem = pl.BlockSpec(memory_space=pltpu.VMEM)
    hbm = pl.BlockSpec(memory_space=pltpu.HBM)
    block = (levels, rows, lanes)
    line = (levels, lanes)
    strip = (levels, group, lanes)
    shapes = [
        strip, (levels, rows - 2 * group, lanes), strip,
        strip, (levels, rows - 2 * group, lanes), strip,
        (6,) + line, (6,) + line, (10,) + line, (5,) + line, (5,) + line, (6,) + line,
        (group, lanes), (group, lanes), (nlon, 6) + line,
    ]
    tall = (levels * pitch + pad, lanes)
    turned = (blocks, lanes + 2 * pad, lanes)
    packs = (chunks, 11, blocks_in, lanes)
    dma = pltpu.SemaphoreType.DMA
    V = pltpu.VMEM
    fields = pl.pallas_call(
        functools.partial(exchange_kernel, nlat, nlon, levels, rows),
        out_shape=[V(s, f32) for s in shapes],
        in_specs=[hbm] * 8,
        out_specs=[vmem] * len(shapes),
        scratch_shapes=[
            V((4,) + block, f32), V((2,) + block, jnp.int32), V((2, rows, lanes), f32),
            V((4, 4) + line, f32), V((2, 4) + line, jnp.int32),
            V(tall, f32), V(tall, f32), V(block, f32), V(block, f32), V(block, f32),
            V(turned, f32), V(turned, f32), V(turned, f32),
            V(packs, f32), V(packs, f32),
            V((group, lanes), f32), V((sides, group, lanes), f32),
            V((chunks, blocks_in, lanes), f32),
            dma((3,)), dma((loads, 2)),
            dma, dma, dma, dma,
            dma((sides,)), dma((chunks, sides)), dma((sides,)), dma((sides,)), dma((2,)), dma((2,)),
            dma((nlon,)), dma((nlon,)),
        ],
        compiler_params=pltpu.CompilerParams(
            collective_id=0, has_side_effects=True, vmem_limit_bytes=36 * 1024 * 1024
        ),
        name="exchange",
    )(u, v, eu, ev, su, sv, mu, mv)
    u_low, u_mid, u_high, v_low, v_mid, v_high = fields[:6]
    low_own, high_own, keep, side, up_in, down_in, corner_u, corner_v, band = fields[6:]
    changed = (u_low, u_high, v_low, v_high, down_in)
    fixed = (u_mid, v_mid, low_own, high_own, keep, side, up_in, corner_u, corner_v, band)
    result = pl.pallas_call(
        functools.partial(finish_kernel, nlat, nlon, levels, rows),
        out_shape=[jax.ShapeDtypeStruct(block, f32)] * 2 + [V(x.shape, f32) for x in changed],
        in_specs=[pl.BlockSpec(memory_space=pltpu.SMEM)] + [vmem] * (len(fixed) + len(changed)),
        out_specs=[hbm] * 2 + [vmem] * len(changed),
        input_output_aliases={1 + len(fixed) + k: 2 + k for k in range(len(changed))},
        scratch_shapes=[V(line, f32), dma((6,))],
        compiler_params=pltpu.CompilerParams(vmem_limit_bytes=16 * 1024 * 1024),
        name="finish",
    )(fold, *fixed, *changed)
    return tuple(result[:2])


def solution(mesh):
    level_rows_columns = P(None, "lat", "lon")
    return jax.shard_map(
        functools.partial(local, mesh.shape["lat"], mesh.shape["lon"]),
        mesh=mesh,
        in_specs=(
            level_rows_columns,
            level_rows_columns,
            level_rows_columns,
            level_rows_columns,
            P("lat", "lon"),
            P("lat", "lon"),
            level_rows_columns,
            level_rows_columns,
            P(),
        ),
        out_specs=(level_rows_columns,) * 2,
        check_vma=False,
    )
```
